32 devices in a mesh: grp: 4 (over y, x), row: 8 (over z, core).
Axes of the slice: x: 2, y: 2, z: 4, core: 2. Of those that a mesh axis runs over, the one named last changes fastest.
Arguments:
- embeds: bfloat16 [4096, 384], P(('grp', 'row')), may hold values from -6 to 6
- w_hidden: bfloat16 [384, 384], replicated, may hold values from -0.3125 to 0.3125
- b_hidden: float32 [384], replicated, may hold values from -3 to 3
- w_out: bfloat16 [384, 128], replicated, may hold values from -0.3125 to 0.3125
- probes: int32 [16, 4096], P(None, ('grp', 'row')), may hold values from 0 to 1
Outputs:
- solves: float32 [16, 4096], P(None, ('grp', 'row'))
- logdet_rate: float32 [16], replicated
- scale_grad: float32 [16], replicated
The draws below stay inside these ranges and needn't reach their ends.
All inputs are finite; a program needn't handle non-finite values.
Results may differ from the reference program's by a relative error of at most 0.0085.
Values may be sent and summed in bfloat16 or wider, within the bound.
No kernel may reach another device: no remote copies, remote signals or barrier semaphores. Data moves between devices by JAX's collectives and lax.ppermute only.
A program may use at most 128 MiB of HBM per device.

```python
import math
import jax
import jax.numpy as jnp
from jax import lax

EMB = 384
FEAT = 128
PROBES = 16
ITERS = 8
SWEEPS = 6
ROWS = 4096


def draw_embeds(key, part):
    key_perm, key_center, key_jitter, key_scale = jax.random.split(jax.random.fold_in(key, 11), 4)
    copies = 8
    shuffled = jax.random.permutation(key_perm, ROWS)
    members = shuffled // copies
    group_count = ROWS // copies
    centers = jax.random.normal(key_center, (group_count, EMB), jnp.float32)
    jitter = 0.35 * jax.random.normal(key_jitter, (ROWS, EMB), jnp.float32)
    embeds = centers[members] + jitter
    return jnp.clip(embeds, -6.0, 6.0).astype(jnp.bfloat16)


def place_ends(result, own_key, least, high):
    longest = result.shape.index(max(result.shape))
    spots = []
    for shift in (0, 1):
        where = [jax.random.randint(jax.random.fold_in(own_key, axis), (), 0, length) for axis, length in enumerate(result.shape)]
        where[longest] = (where[longest] + shift) % result.shape[longest]
        spots.append(tuple(where))
    return result.at[spots[0]].set(least).at[spots[1]].set(high)


def centred(stream_key, extent, width, reach, kind=jnp.bfloat16):
    return jnp.clip(width * jax.random.normal(stream_key, extent, jnp.float32), -reach, reach).astype(kind)


def setup_inputs(seed: int = 0) -> dict:
    keys = jax.random.split(jax.random.key(seed), 6)
    embeds = draw_embeds(jax.random.fold_in(keys[5], 71), 0)
    w_hidden = centred(keys[1], (EMB, EMB), EMB ** -0.5, 0.3125)
    b_hidden = centred(keys[2], (EMB,), 0.5, 3.0, jnp.float32)
    w_out = centred(keys[3], (EMB, FEAT), EMB ** -0.5, 0.3125)
    probes = place_ends(jax.random.randint(keys[4], (PROBES, ROWS), 0, 2), jax.random.fold_in(keys[4], 1), 0, 1).astype(jnp.int32)
    return dict(embeds=embeds, w_hidden=w_hidden, b_hidden=b_hidden, w_out=w_out, probes=probes)


INV_WIDTH = 1.0 / 12.0
NOISE_LEVEL = 0.5
FLOOR_BETA = 0.01
EIGEN_FLOOR = 0.25

def rotate(matrix, vectors, first_idx, second_idx):
    diag_first = matrix[first_idx, first_idx]
    diag_second = matrix[second_idx, second_idx]
    off_value = matrix[first_idx, second_idx]
    half_angle = 0.5 * jnp.arctan2(2.0 * off_value, diag_first - diag_second)
    cosine = jnp.cos(half_angle)
    sine_val = jnp.sin(half_angle)
    row_first = matrix[first_idx]
    row_second = matrix[second_idx]
    matrix = matrix.at[first_idx].set(cosine * row_first + sine_val * row_second)
    matrix = matrix.at[second_idx].set(cosine * row_second - sine_val * row_first)
    col_first = matrix[:, first_idx]
    col_second = matrix[:, second_idx]
    matrix = matrix.at[:, first_idx].set(cosine * col_first + sine_val * col_second)
    matrix = matrix.at[:, second_idx].set(cosine * col_second - sine_val * col_first)
    vec_first = vectors[:, first_idx]
    vec_second = vectors[:, second_idx]
    vectors = vectors.at[:, first_idx].set(cosine * vec_first + sine_val * vec_second)
    vectors = vectors.at[:, second_idx].set(cosine * vec_second - sine_val * vec_first)
    return (matrix, vectors)

def quadrature(alphas, betas):
    tri_order = alphas.shape[0]
    identity = jnp.eye(tri_order, dtype=jnp.float32)
    upper_band = jnp.concatenate([jnp.zeros_like(alphas[:1]), betas], axis=0)
    shifted = jnp.eye(tri_order, k=1, dtype=jnp.float32)[:, :, None] * upper_band[None, :, :]
    matrix = identity[:, :, None] * alphas[None, :, :] + shifted + jnp.transpose(shifted, (1, 0, 2))
    vectors = jnp.broadcast_to(identity[:, :, None], matrix.shape) + jnp.zeros_like(matrix)
    for sweep_index in range(SWEEPS):
        for first_idx in range(tri_order):
            for second_idx in range(first_idx + 1, tri_order):
                matrix, vectors = rotate(matrix, vectors, first_idx, second_idx)
    eigenvalues = jnp.maximum(lax.optimization_barrier(jnp.sum(matrix * identity[:, :, None], axis=1)), EIGEN_FLOOR)
    leading = vectors[0]
    logdet = lax.optimization_barrier(jnp.sum(jnp.square(leading) * jnp.log(eigenvalues), axis=0))
    coefficients = lax.optimization_barrier(jnp.sum(vectors * (leading / eigenvalues)[None, :, :], axis=1))
    scale_grad = 1.0 - NOISE_LEVEL * coefficients[0]
    return (logdet, scale_grad, coefficients)

def apply_kernel(features, norms_all, vectors_low):
    total_rows = features.shape[0]
    block_rows = math.gcd(total_rows, 512)
    block_count = total_rows // block_rows
    feats_wide = features.astype(jnp.float32)
    vectors_wide = vectors_low.astype(jnp.float32)

    def one_block(block_index):
        row_block = lax.dynamic_slice_in_dim(feats_wide, block_index * block_rows, block_rows, 0)
        norm_block = lax.dynamic_slice_in_dim(norms_all, block_index * block_rows, block_rows, 0)
        inner = jnp.dot(row_block, feats_wide.T, precision=lax.Precision.HIGHEST)
        distance = norm_block[:, None] + norms_all[None, :] - 2.0 * inner
        kernel_low = jnp.exp(-jnp.maximum(distance, 0.0) * INV_WIDTH).astype(jnp.bfloat16)
        kernel_tile = lax.optimization_barrier(kernel_low).astype(jnp.float32)
        return jnp.dot(vectors_wide, kernel_tile.T, precision=lax.Precision.HIGHEST)
    stacked = lax.map(one_block, jnp.arange(block_count, dtype=jnp.int32))
    return jnp.transpose(stacked, (1, 0, 2)).reshape(vectors_low.shape[0], total_rows)

def reference(embeds, w_hidden, b_hidden, w_out, probes):
    hidden = jax.nn.gelu(jnp.dot(embeds, w_hidden, preferred_element_type=jnp.float32) + b_hidden).astype(jnp.bfloat16)
    features = jnp.dot(hidden, w_out, preferred_element_type=jnp.float32).astype(jnp.bfloat16)
    norms_all = lax.optimization_barrier(jnp.sum(jnp.square(features.astype(jnp.float32)), axis=1))
    scale_root = math.sqrt(ROWS)
    current = (2 * probes - 1).astype(jnp.float32) / scale_root
    previous = jnp.zeros_like(current)
    beta_prev = jnp.zeros((current.shape[0],), jnp.float32)
    basis_list = []
    alpha_list = []
    beta_list = []
    for iteration in range(ITERS):
        kernel_image = apply_kernel(features, norms_all, current.astype(jnp.bfloat16)) + NOISE_LEVEL * current
        alpha_now = lax.optimization_barrier(jnp.sum(current * kernel_image, axis=1))
        residual = kernel_image - alpha_now[:, None] * current - beta_prev[:, None] * previous
        basis_list.append(current)
        alpha_list.append(alpha_now)
        if iteration + 1 < ITERS:
            residual_sq = lax.optimization_barrier(jnp.sum(residual * residual, axis=1))
            beta_now = jnp.sqrt(jnp.maximum(residual_sq, 0.0) + FLOOR_BETA)
            beta_list.append(beta_now)
            previous = current
            current = residual / beta_now[:, None]
            beta_prev = beta_now
    logdet, scale_grad, coefficients = quadrature(jnp.stack(alpha_list), jnp.stack(beta_list))
    solves = scale_root * jnp.einsum('jp,jpn->pn', coefficients, jnp.stack(basis_list))
    return (solves, logdet, scale_grad)
```

```python
import functools
import math

import jax
import jax.numpy as jnp
from jax import lax
from jax.experimental import pallas as pl
from jax.experimental.pallas import tpu as pltpu
from jax.sharding import PartitionSpec as P

ITERS = 8
SWEEPS = 6
INV_WIDTH = 1.0 / 12.0
NOISE_LEVEL = 0.5
FLOOR_BETA = 0.01
EIGEN_FLOOR = 0.25
LANES = 128
VMEM_KERNEL_BYTES = 40 * 2**20


def head_kernel(embeds_ref, w_hidden_ref, b_hidden_ref, w_out_ref, probes_ref, out_ref):
    rows = embeds_ref.shape[0]
    hidden = jax.nn.gelu(
        jnp.dot(embeds_ref[...], w_hidden_ref[...], preferred_element_type=jnp.float32)
        + b_hidden_ref[...]
    ).astype(jnp.bfloat16)
    out_ref[:rows, :] = jnp.dot(
        hidden, w_out_ref[...], preferred_element_type=jnp.float32
    ).astype(jnp.bfloat16)
    out_ref[rows:, :] = probes_ref[...].astype(jnp.float32).astype(jnp.bfloat16)


def head(embeds, w_hidden, b_hidden, w_out, probes):
    rows, feat = embeds.shape[0], w_out.shape[1]
    return pl.pallas_call(
        head_kernel,
        out_shape=jax.ShapeDtypeStruct((rows + probes.shape[0], feat), jnp.bfloat16),
    )(embeds, w_hidden, b_hidden[None, :], w_out, probes)


def swap(value, axis, flip):
    size = lax.axis_size(axis)
    return lax.ppermute(value, axis, [(i, i ^ flip) for i in range(size)])


def gather_all(block):
    half = lax.axis_size("row") // 2
    pieces = [block] + [swap(block, "row", 2 * k) for k in range(1, half)]
    line = jnp.stack(pieces)
    groups = [line] + [swap(line, "grp", k) for k in range(1, lax.axis_size("grp"))]
    own = jnp.concatenate(groups)
    return own, swap(own, "row", 1)


def pairs_of_round(order, turn):
    ring = order - 1
    pairs = [(ring, turn)]
    for gap in range(1, order // 2):
        pairs.append(((turn + gap) % ring, (turn - gap) % ring))
    return [tuple(sorted(pair)) for pair in pairs]


def jacobi_round(entries, columns, pairs):
    entries, columns = dict(entries), list(columns)

    def key(i, j):
        return (i, j) if i <= j else (j, i)

    turns = []
    for p, q in pairs:
        off = entries[p, q]
        gap = entries[q, q] - entries[p, p]
        root = jnp.abs(gap) + jnp.sqrt(gap * gap + 4.0 * off * off)
        numer = jnp.where(gap >= 0.0, 2.0 * off, -2.0 * off)
        tangent = jnp.where(root > 0.0, numer / jnp.where(root > 0.0, root, 1.0), 0.0)
        cosine = lax.rsqrt(1.0 + tangent * tangent)
        turns.append((cosine, cosine * tangent, tangent * off))
    for (p, q), (cosine, sine, shift) in zip(pairs, turns):
        entries[p, p] = entries[p, p] - shift
        entries[q, q] = entries[q, q] + shift
        entries[p, q] = jnp.zeros_like(shift)
        col_p, col_q = columns[p], columns[q]
        columns[p] = cosine * col_p - sine * col_q
        columns[q] = sine * col_p + cosine * col_q
    for a in range(len(pairs)):
        for b in range(a + 1, len(pairs)):
            (p, q), (r, s) = pairs[a], pairs[b]
            cos_a, sin_a, _ = turns[a]
            cos_b, sin_b, _ = turns[b]
            pr, ps = entries[key(p, r)], entries[key(p, s)]
            qr, qs = entries[key(q, r)], entries[key(q, s)]
            pr, qr = cos_a * pr - sin_a * qr, sin_a * pr + cos_a * qr
            ps, qs = cos_a * ps - sin_a * qs, sin_a * ps + cos_a * qs
            pr, ps = cos_b * pr - sin_b * ps, sin_b * pr + cos_b * ps
            qr, qs = cos_b * qr - sin_b * qs, sin_b * qr + cos_b * qs
            entries[key(p, r)], entries[key(p, s)] = pr, ps
            entries[key(q, r)], entries[key(q, s)] = qr, qs
    return entries, columns


def quadrature_lanes(alphas, betas, order):
    shape = alphas[0].shape
    keys = [(i, j) for i in range(order) for j in range(i, order)]
    entries = {}
    for i, j in keys:
        if i == j:
            entries[i, j] = alphas[i]
        elif j == i + 1:
            entries[i, j] = betas[i]
        else:
            entries[i, j] = jnp.zeros(shape, jnp.float32)
    sublane = lax.broadcasted_iota(jnp.int32, shape, 0)
    columns = [jnp.where(sublane == k, 1.0, 0.0).astype(jnp.float32) for k in range(order)]

    def sweep(_, state):
        values, columns = state
        entries = dict(zip(keys, values))
        for turn in range(order - 1):
            entries, columns = jacobi_round(entries, columns, pairs_of_round(order, turn))
        return tuple(entries[k] for k in keys), tuple(columns)

    values, columns = lax.fori_loop(
        0, SWEEPS, sweep, (tuple(entries[k] for k in keys), tuple(columns))
    )
    entries = dict(zip(keys, values))
    logdet = jnp.zeros((1, shape[1]), jnp.float32)
    coef = jnp.zeros(shape, jnp.float32)
    for k in range(order):
        eigen = jnp.maximum(entries[k, k][:1], EIGEN_FLOOR)
        leading = columns[k][:1]
        logdet = logdet + leading * leading * jnp.log(eigen)
        coef = coef + columns[k] * (leading / eigen)
    return logdet, coef


def split3(value):
    high = value.astype(jnp.bfloat16)
    rest = value - high.astype(jnp.float32)
    mid = rest.astype(jnp.bfloat16)
    low = (rest - mid.astype(jnp.float32)).astype(jnp.bfloat16)
    return high, mid, low


def lanczos_kernel(
    place_ref, own_ref, oth_ref, solves_ref, stats_ref, left, right, kern, basis, image, tri, *, lines
):
    half, block_rows, feat = own_ref.shape
    probes = solves_ref.shape[0]
    local = block_rows - probes
    rows = kern.shape[0]
    root = math.sqrt(rows)
    side, group, line = place_ref[0], place_ref[1], place_ref[2]

    def slot_of(index, other):
        near = jnp.bitwise_xor(group, index // lines) * lines + jnp.bitwise_xor(line, index % lines)
        return (side + other - 2 * side * other) * half + near

    lane = lax.broadcasted_iota(jnp.int32, (local, LANES), 1)

    def assemble(index, ref, other):
        start = pl.multiple_of(slot_of(index, other) * local, local)
        feats = ref[index, :local, :]
        wide = feats.astype(jnp.float32)
        high, mid, low = split3(-0.5 * jnp.sum(wide * wide, axis=1, keepdims=True))
        one = jnp.ones_like(high)

        def extra(parts):
            total = jnp.zeros((local, LANES), jnp.float32)
            for k, part in enumerate(parts):
                total = jnp.where(lane == k, part.astype(jnp.float32), total)
            return total.astype(jnp.bfloat16)

        left[pl.ds(start, local), :feat] = feats
        left[pl.ds(start, local), feat:] = extra((high, mid, low, one, one, one))
        right[pl.ds(start, local), :feat] = feats
        right[pl.ds(start, local), feat:] = extra((one, one, one, high, mid, low))
        bits = ref[index, local:, :].astype(jnp.float32)
        basis[1, :, pl.ds(start, local)] = (2.0 * bits - 1.0) / root

    def assemble_both(index, carry):
        assemble(index, own_ref, 0)
        assemble(index, oth_ref, 1)
        return carry

    lax.fori_loop(0, half, assemble_both, 0)

    width, height = 256, 512

    def form(step, carry):
        start = pl.multiple_of(step * width, width)
        cols = right[pl.ds(start, width), :]
        for top in range(0, rows, height):
            inner = lax.dot_general(
                left[top : top + height, :],
                cols,
                (((1,), (1,)), ((), ())),
                preferred_element_type=jnp.float32,
            )
            kern[top : top + height, pl.ds(start, width)] = jnp.exp(
                jnp.minimum(inner, 0.0) * (2.0 * INV_WIDTH)
            ).astype(jnp.bfloat16)
        return carry

    lax.fori_loop(0, rows // width, form, 0)

    basis[0] = jnp.zeros_like(basis[0])
    tri[...] = jnp.zeros_like(tri)
    table_lane = lax.broadcasted_iota(jnp.int32, (probes, LANES), 1)
    chunk = 1024

    def lanczos(step, beta_prev):
        current = basis[step + 1]
        low = current.astype(jnp.bfloat16)
        alpha = jnp.zeros((probes, 1), jnp.float32)
        for start in range(0, rows, chunk):
            here = slice(start, start + chunk)
            part = jnp.dot(low, kern[:, here], preferred_element_type=jnp.float32)
            mine = basis[step + 1, :, here]
            part = part + NOISE_LEVEL * mine
            image[:, here] = part
            alpha = alpha + jnp.sum(mine * part, axis=1, keepdims=True)
        residual = image[...] - alpha * current - beta_prev * basis[step]
        beta = jnp.sqrt(
            jnp.maximum(jnp.sum(residual * residual, axis=1, keepdims=True), 0.0) + FLOOR_BETA
        )
        basis[step + 2] = residual / beta
        tri[:probes, :] = jnp.where(
            table_lane == step,
            alpha,
            jnp.where(table_lane == step + ITERS, beta, tri[:probes, :]),
        )
        return beta

    lax.fori_loop(0, ITERS, lanczos, jnp.zeros((probes, 1), jnp.float32))

    turned = jnp.transpose(tri[...])
    spread = lambda j: jnp.broadcast_to(turned[j : j + 1, :], (8, LANES))
    logdet, coef = quadrature_lanes(
        [spread(j) for j in range(ITERS)], [spread(ITERS + j) for j in range(ITERS - 1)], ITERS
    )
    stats_ref[0:1, :] = logdet
    stats_ref[1:2, :] = 1.0 - NOISE_LEVEL * coef[0:1, :]
    tri[:ITERS, :] = coef
    weights = jnp.transpose(tri[...])[:probes, :]
    mine = pl.multiple_of(slot_of(0, 0) * local, local)
    total = jnp.zeros((probes, local), jnp.float32)
    for j in range(ITERS):
        total = total + weights[:, j : j + 1] * basis[j + 1, :, pl.ds(mine, local)]
    solves_ref[...] = root * total


def lanczos(own, oth, probes):
    half, block_rows, feat = own.shape
    local = block_rows - probes
    rows = 2 * half * local
    pairs = lax.axis_index("row")
    place = jnp.stack([pairs % 2, lax.axis_index("grp"), pairs // 2]).astype(jnp.int32)
    vmem = pl.BlockSpec(memory_space=pltpu.VMEM)
    return pl.pallas_call(
        functools.partial(lanczos_kernel, lines=lax.axis_size("row") // 2),
        out_shape=(
            jax.ShapeDtypeStruct((probes, local), jnp.float32),
            jax.ShapeDtypeStruct((8, LANES), jnp.float32),
        ),
        in_specs=[pl.BlockSpec(memory_space=pltpu.SMEM), vmem, vmem],
        out_specs=(vmem, vmem),
        scratch_shapes=[
            pltpu.VMEM((rows, feat + LANES), jnp.bfloat16),
            pltpu.VMEM((rows, feat + LANES), jnp.bfloat16),
            pltpu.VMEM((rows, rows), jnp.bfloat16),
            pltpu.VMEM((ITERS + 2, probes, rows), jnp.float32),
            pltpu.VMEM((probes, rows), jnp.float32),
            pltpu.VMEM((LANES, LANES), jnp.float32),
        ],
        compiler_params=pltpu.CompilerParams(vmem_limit_bytes=56 * 2**20),
    )(place, own, oth)


def replicated(embeds, w_hidden, b_hidden, w_out, probes):
    own, oth = gather_all(head(embeds, w_hidden, b_hidden, w_out, probes))
    solves, stats = lanczos(own, oth, probes.shape[0])
    return solves, stats[0, : probes.shape[0]], stats[1, : probes.shape[0]]


def rotate(matrix, vectors, first_idx, second_idx):
    diag_first = matrix[first_idx, first_idx]
    diag_second = matrix[second_idx, second_idx]
    off_value = matrix[first_idx, second_idx]
    half_angle = 0.5 * jnp.arctan2(2.0 * off_value, diag_first - diag_second)
    cosine = jnp.cos(half_angle)
    sine_val = jnp.sin(half_angle)
    row_first = matrix[first_idx]
    row_second = matrix[second_idx]
    matrix = matrix.at[first_idx].set(cosine * row_first + sine_val * row_second)
    matrix = matrix.at[second_idx].set(cosine * row_second - sine_val * row_first)
    col_first = matrix[:, first_idx]
    col_second = matrix[:, second_idx]
    matrix = matrix.at[:, first_idx].set(cosine * col_first + sine_val * col_second)
    matrix = matrix.at[:, second_idx].set(cosine * col_second - sine_val * col_first)
    vec_first = vectors[:, first_idx]
    vec_second = vectors[:, second_idx]
    vectors = vectors.at[:, first_idx].set(cosine * vec_first + sine_val * vec_second)
    vectors = vectors.at[:, second_idx].set(cosine * vec_second - sine_val * vec_first)
    return (matrix, vectors)


def quadrature(alphas, betas):
    tri_order = alphas.shape[0]
    identity = jnp.eye(tri_order, dtype=jnp.float32)
    upper_band = jnp.concatenate([jnp.zeros_like(alphas[:1]), betas], axis=0)
    shifted = jnp.eye(tri_order, k=1, dtype=jnp.float32)[:, :, None] * upper_band[None, :, :]
    matrix = identity[:, :, None] * alphas[None, :, :] + shifted + jnp.transpose(shifted, (1, 0, 2))
    vectors = jnp.broadcast_to(identity[:, :, None], matrix.shape)
    for sweep_index in range(SWEEPS):
        for first_idx in range(tri_order):
            for second_idx in range(first_idx + 1, tri_order):
                matrix, vectors = rotate(matrix, vectors, first_idx, second_idx)
    eigenvalues = jnp.maximum(jnp.sum(matrix * identity[:, :, None], axis=1), EIGEN_FLOOR)
    leading = vectors[0]
    logdet = jnp.sum(jnp.square(leading) * jnp.log(eigenvalues), axis=0)
    coefficients = jnp.sum(vectors * (leading / eigenvalues)[None, :, :], axis=1)
    scale_grad = 1.0 - NOISE_LEVEL * coefficients[0]
    return (logdet, scale_grad, coefficients)


def kernel_block(row_feats, row_norms, col_block, norm_block):
    inner = lax.dot_general(
        row_feats, col_block, (((1,), (1,)), ((), ())), preferred_element_type=jnp.float32
    )
    distance = row_norms[:, None] + norm_block[None, :] - 2.0 * inner
    return jnp.exp(-jnp.maximum(distance, 0.0) * INV_WIDTH).astype(jnp.bfloat16)


def block_width():
    return 512


def form_tile(row_feats, row_norms, col_feats, col_norms):
    total_cols = col_feats.shape[0]
    step_cols = block_width()
    block_count = total_cols // step_cols

    def one_block(block_index, tile):
        offset = block_index * step_cols
        col_block = lax.dynamic_slice_in_dim(col_feats, offset, step_cols, 0)
        norm_block = lax.dynamic_slice_in_dim(col_norms, offset, step_cols, 0)
        block = kernel_block(row_feats, row_norms, col_block, norm_block)
        return lax.dynamic_update_slice_in_dim(tile, block, offset, 1)

    empty = jnp.zeros((row_feats.shape[0], total_cols), jnp.bfloat16)
    return lax.fori_loop(0, block_count, one_block, empty)


def apply_kernel(vectors_low, tile):
    partial_value = lax.dot_general(
        lax.all_gather(vectors_low, "row", axis=1, tiled=True),
        tile,
        (((1,), (1,)), ((), ())),
        preferred_element_type=jnp.float32,
    )
    return lax.psum_scatter(partial_value, "grp", scatter_dimension=1, tiled=True)


def distributed(embeds, w_hidden, b_hidden, w_out, probes):
    hidden = jax.nn.gelu(
        jnp.dot(embeds, w_hidden, preferred_element_type=jnp.float32) + b_hidden
    ).astype(jnp.bfloat16)
    features = jnp.dot(hidden, w_out, preferred_element_type=jnp.float32).astype(jnp.bfloat16)
    row_feats = lax.all_gather(features, "grp", axis=0, tiled=True)
    col_feats = lax.all_gather(features, "row", axis=0, tiled=True)
    row_norms = jnp.sum(jnp.square(row_feats.astype(jnp.float32)), axis=1)
    col_norms = jnp.sum(jnp.square(col_feats.astype(jnp.float32)), axis=1)
    tile = form_tile(row_feats, row_norms, col_feats, col_norms)
    total_rows = probes.shape[1] * lax.axis_size("grp") * lax.axis_size("row")
    scale_root = math.sqrt(total_rows)
    current = (2 * probes - 1).astype(jnp.float32) / scale_root
    previous = jnp.zeros_like(current)
    beta_prev = jnp.zeros((current.shape[0],), jnp.float32)
    basis_list = []
    alpha_list = []
    beta_list = []
    for iteration in range(ITERS):
        kernel_image = apply_kernel(current.astype(jnp.bfloat16), tile) + NOISE_LEVEL * current
        moments = jnp.stack(
            [
                jnp.sum(current * kernel_image, axis=1),
                jnp.sum(kernel_image * kernel_image, axis=1),
                jnp.sum(previous * kernel_image, axis=1),
                jnp.sum(current * previous, axis=1),
                jnp.sum(current * current, axis=1),
                jnp.sum(previous * previous, axis=1),
            ]
        )
        moments = lax.psum(moments, ("grp", "row"))
        alpha_now = moments[0]
        residual_sq = (
            moments[1]
            + alpha_now * alpha_now * moments[4]
            + beta_prev * beta_prev * moments[5]
            - 2.0 * alpha_now * moments[0]
            - 2.0 * beta_prev * moments[2]
            + 2.0 * alpha_now * beta_prev * moments[3]
        )
        residual = kernel_image - alpha_now[:, None] * current - beta_prev[:, None] * previous
        basis_list.append(current)
        alpha_list.append(alpha_now)
        if iteration + 1 < ITERS:
            beta_now = jnp.sqrt(jnp.maximum(residual_sq, 0.0) + FLOOR_BETA)
            beta_list.append(beta_now)
            previous = current
            current = residual / beta_now[:, None]
            beta_prev = beta_now
    logdet, scale_grad, coefficients = quadrature(jnp.stack(alpha_list), jnp.stack(beta_list))
    solves = scale_root * jnp.einsum("jp,jpn->pn", coefficients, jnp.stack(basis_list))
    return (solves, logdet, scale_grad)


def power_of_two(value):
    return value & (value - 1) == 0


def solution(mesh):
    groups, lines = mesh.shape["grp"], mesh.shape["row"]

    def local(embeds, w_hidden, b_hidden, w_out, probes):
        rows = embeds.shape[0] * groups * lines
        fits = (
            2 * rows * rows <= VMEM_KERNEL_BYTES
            and lines % 2 == 0
            and power_of_two(groups)
            and power_of_two(lines)
            and probes.shape[1] == LANES
            and w_out.shape[1] == LANES
            and probes.shape[0] % 16 == 0
        )
        step = replicated if fits else distributed
        return step(embeds, w_hidden, b_hidden, w_out, probes)

    return jax.shard_map(
        local,
        mesh=mesh,
        in_specs=(P(("grp", "row"), None), P(), P(), P(), P(None, ("grp", "row"))),
        out_specs=(P(None, ("grp", "row")), P(), P()),
        check_vma=False,
    )
```

```python
import functools
import math

import jax
import jax.numpy as jnp
from jax import lax
from jax.experimental import pallas as pl
from jax.experimental.pallas import tpu as pltpu
from jax.sharding import PartitionSpec as P

ITERS = 8
SWEEPS = 6
INV_WIDTH = 1.0 / 12.0
NOISE_LEVEL = 0.5
FLOOR_BETA = 0.01
EIGEN_FLOOR = 0.25
LANES = 128
KERNEL_BYTES = 40 * 2**20


def head_kernel(embeds_ref, w_hidden_ref, b_hidden_ref, w_out_ref, probes_ref, out_ref):
    rows = embeds_ref.shape[0]
    hidden = jax.nn.gelu(
        jnp.dot(embeds_ref[...], w_hidden_ref[...], preferred_element_type=jnp.float32)
        + b_hidden_ref[...][None, :]
    ).astype(jnp.bfloat16)
    out_ref[:rows, :] = jnp.dot(
        hidden, w_out_ref[...], preferred_element_type=jnp.float32
    ).astype(jnp.bfloat16)
    out_ref[rows:, :] = probes_ref[...].astype(jnp.float32).astype(jnp.bfloat16)


def head(embeds, w_hidden, b_hidden, w_out, probes):
    rows, feat = embeds.shape[0], w_out.shape[1]
    return pl.pallas_call(
        head_kernel,
        out_shape=jax.ShapeDtypeStruct((rows + probes.shape[0], feat), jnp.bfloat16),
    )(embeds, w_hidden, b_hidden, w_out, probes)


def swap(value, axis, flip):
    size = lax.axis_size(axis)
    return lax.ppermute(value, axis, [(i, i ^ flip) for i in range(size)])


def gather_half(block):
    half = lax.axis_size("row") // 2
    pieces = [block] + [swap(block, "row", 2 * k) for k in range(1, half)]
    line = jnp.stack(pieces)
    return jnp.concatenate([line] + [swap(line, "grp", k) for k in range(1, lax.axis_size("grp"))])


def partner(value):
    return swap(value, "row", 1)


def pairs_of_round(order, turn):
    ring = order - 1
    pairs = [(ring, turn)]
    for gap in range(1, order // 2):
        pairs.append(((turn + gap) % ring, (turn - gap) % ring))
    return [tuple(sorted(pair)) for pair in pairs]


def jacobi_round(entries, columns, pairs):
    entries, columns = dict(entries), list(columns)

    def key(i, j):
        return (i, j) if i <= j else (j, i)

    turns = []
    for p, q in pairs:
        off = entries[p, q]
        gap = entries[q, q] - entries[p, p]
        root = jnp.abs(gap) + jnp.sqrt(gap * gap + 4.0 * off * off)
        numer = jnp.where(gap >= 0.0, 2.0 * off, -2.0 * off)
        tangent = jnp.where(root > 0.0, numer / jnp.where(root > 0.0, root, 1.0), 0.0)
        cosine = lax.rsqrt(1.0 + tangent * tangent)
        turns.append((cosine, cosine * tangent, tangent * off))
    for (p, q), (cosine, sine, shift) in zip(pairs, turns):
        entries[p, p] = entries[p, p] - shift
        entries[q, q] = entries[q, q] + shift
        entries[p, q] = jnp.zeros_like(shift)
        col_p, col_q = columns[p], columns[q]
        columns[p] = cosine * col_p - sine * col_q
        columns[q] = sine * col_p + cosine * col_q
    for a in range(len(pairs)):
        for b in range(a + 1, len(pairs)):
            (p, q), (r, s) = pairs[a], pairs[b]
            cos_a, sin_a, _ = turns[a]
            cos_b, sin_b, _ = turns[b]
            pr, ps = entries[key(p, r)], entries[key(p, s)]
            qr, qs = entries[key(q, r)], entries[key(q, s)]
            pr, qr = cos_a * pr - sin_a * qr, sin_a * pr + cos_a * qr
            ps, qs = cos_a * ps - sin_a * qs, sin_a * ps + cos_a * qs
            pr, ps = cos_b * pr - sin_b * ps, sin_b * pr + cos_b * ps
            qr, qs = cos_b * qr - sin_b * qs, sin_b * qr + cos_b * qs
            entries[key(p, r)], entries[key(p, s)] = pr, ps
            entries[key(q, r)], entries[key(q, s)] = qr, qs
    return entries, columns


def quadrature_lanes(alphas, betas, order):
    shape = alphas[0].shape
    keys = [(i, j) for i in range(order) for j in range(i, order)]
    entries = {}
    for i, j in keys:
        if i == j:
            entries[i, j] = alphas[i]
        elif j == i + 1:
            entries[i, j] = betas[i]
        else:
            entries[i, j] = jnp.zeros(shape, jnp.float32)
    sublane = lax.broadcasted_iota(jnp.int32, shape, 0)
    columns = [jnp.where(sublane == k, 1.0, 0.0).astype(jnp.float32) for k in range(order)]

    def sweep(_, state):
        values, columns = state
        entries = dict(zip(keys, values))
        for turn in range(order - 1):
            entries, columns = jacobi_round(entries, columns, pairs_of_round(order, turn))
        return tuple(entries[k] for k in keys), tuple(columns)

    values, columns = lax.fori_loop(
        0, SWEEPS, sweep, (tuple(entries[k] for k in keys), tuple(columns))
    )
    entries = dict(zip(keys, values))
    logdet = jnp.zeros((1, shape[1]), jnp.float32)
    coef = jnp.zeros(shape, jnp.float32)
    for k in range(order):
        eigen = jnp.maximum(entries[k, k][:1], EIGEN_FLOOR)
        leading = columns[k][:1]
        logdet = logdet + leading * leading * jnp.log(eigen)
        coef = coef + columns[k] * (leading / eigen)
    return logdet, coef


def split3(value):
    high = value.astype(jnp.bfloat16)
    rest = value - high.astype(jnp.float32)
    mid = rest.astype(jnp.bfloat16)
    low = (rest - mid.astype(jnp.float32)).astype(jnp.bfloat16)
    return high, mid, low


def slot_of(index):
    lines = lax.axis_size("row") // 2
    line, group = lax.axis_index("row") // 2, lax.axis_index("grp")
    return (group ^ (index // lines)) * lines + (line ^ (index % lines))


def place_blocks(blocks, left, right, start_vec, probes):
    count, block_rows, feat = blocks.shape
    local = block_rows - probes
    root = math.sqrt(2 * count * local)
    lane = lax.broadcasted_iota(jnp.int32, (local, LANES), 1)

    def extra(parts):
        total = jnp.zeros((local, LANES), jnp.float32)
        for k, part in enumerate(parts):
            total = jnp.where(lane == k, part, total)
        return total.astype(jnp.bfloat16)

    def place(index, carry):
        start = pl.multiple_of(slot_of(index) * local, local)
        feats = blocks[index, :local, :]
        wide = feats.astype(jnp.float32)
        norms = split3(-0.5 * jnp.sum(wide * wide, axis=1, keepdims=True))
        ones = (1.0, 1.0, 1.0)
        left[pl.ds(start, local), :feat] = feats
        left[pl.ds(start, local), feat:] = extra(norms + ones)
        if right is not None:
            right[pl.ds(start, local), :feat] = feats
            right[pl.ds(start, local), feat:] = extra(ones + norms)
        bits = blocks[index, local:, :].astype(jnp.float32)
        start_vec[:, pl.ds(start, local)] = (2.0 * bits - 1.0) / root
        return carry

    lax.fori_loop(0, count, place, 0, unroll=4)


def form(left, right, kern):
    rows, cols = left.shape[0], right.shape[0]
    width, height = 512, 512

    def columns(step, carry):
        start = pl.multiple_of(step * width, width)
        block = right[pl.ds(start, width), :]
        for top in range(0, rows, height):
            inner = lax.dot_general(
                left[top : top + height, :],
                block,
                (((1,), (1,)), ((), ())),
                preferred_element_type=jnp.float32,
            )
            kern[top : top + height, pl.ds(start, width)] = jnp.exp2(
                jnp.minimum(inner, 0.0) * (2.0 * INV_WIDTH * math.log2(math.e))
            ).astype(jnp.bfloat16)
        return carry

    lax.fori_loop(0, cols // width, columns, 0)


def product(own, oth, kern_own, kern_oth, image):
    width = 512
    own, oth = own.astype(jnp.bfloat16), oth.astype(jnp.bfloat16)
    for start in range(0, image.shape[1], width):
        here = slice(start, start + width)
        image[:, here] = jnp.dot(
            own, kern_own[:, here], preferred_element_type=jnp.float32
        ) + jnp.dot(oth, kern_oth[:, here], preferred_element_type=jnp.float32)


def form_own_kernel(blocks, kern, right, start_vec, left):
    place_blocks(blocks, left, right, start_vec, start_vec.shape[0])
    form(left, right, kern)


def form_oth_kernel(blocks, right, kern_own, own_vec, kern, start_vec, image, left):
    place_blocks(blocks, left, None, start_vec, start_vec.shape[0])
    form(left, right, kern)
    product(own_vec[...], start_vec[...], kern_own, kern, image)


def row_sum(first, second):
    return jnp.sum(first * second, axis=1, keepdims=True)


def step_kernel(*refs, step):
    if step > 1:
        before_own, before_oth, table, *refs = refs
    own, oth, image_own, image_oth, kern_own, kern_oth, next_own, next_oth, image, table_out = refs
    lane = lax.broadcasted_iota(jnp.int32, table_out.shape, 1)
    q_own, q_oth = own[...], oth[...]
    w_own = image_own[...] + NOISE_LEVEL * q_own
    w_oth = image_oth[...] + NOISE_LEVEL * q_oth
    alpha = row_sum(q_own, w_own) + row_sum(q_oth, w_oth)
    w_own = w_own - alpha * q_own
    w_oth = w_oth - alpha * q_oth
    if step > 1:
        last = table[...]
        beta = last[:, ITERS + step - 2 : ITERS + step - 1]
        w_own = w_own - beta * before_own[...]
        w_oth = w_oth - beta * before_oth[...]
    else:
        last = jnp.zeros(table_out.shape, jnp.float32)
    beta = jnp.sqrt(
        jnp.maximum(row_sum(w_own, w_own) + row_sum(w_oth, w_oth), 0.0) + FLOOR_BETA
    )
    w_own, w_oth = w_own / beta, w_oth / beta
    next_own[...], next_oth[...] = w_own, w_oth
    table_out[...] = jnp.where(
        lane == step - 1, alpha, jnp.where(lane == ITERS + step - 1, beta, last)
    )
    product(w_own, w_oth, kern_own, kern_oth, image)


def finish_kernel(*refs):
    table, oth, image_own, image_oth, *basis = refs[: 4 + ITERS]
    solves, logdet_ref, scale_ref, square = refs[4 + ITERS :]
    probes, local = solves.shape
    root = math.sqrt(2 * oth.shape[1])
    own = basis[-1]
    alpha = row_sum(own[...], image_own[...] + NOISE_LEVEL * own[...]) + row_sum(
        oth[...], image_oth[...] + NOISE_LEVEL * oth[...]
    )
    lane = lax.broadcasted_iota(jnp.int32, table.shape, 1)
    square[...] = jnp.zeros_like(square)
    square[:probes, :] = jnp.where(lane == ITERS - 1, alpha, table[...])
    turned = jnp.transpose(square[...])
    spread = lambda j: jnp.broadcast_to(turned[j : j + 1, :], (8, LANES))
    logdet, coef = quadrature_lanes(
        [spread(j) for j in range(ITERS)], [spread(ITERS + j) for j in range(ITERS - 1)], ITERS
    )
    logdet_ref[...] = logdet[0, :probes]
    scale_ref[...] = 1.0 - NOISE_LEVEL * coef[0, :probes]
    square[:ITERS, :] = coef
    weights = jnp.transpose(square[...])[:probes, :]
    mine = pl.multiple_of(slot_of(0) * local, local)
    total = jnp.zeros((probes, local), jnp.float32)
    for j in range(ITERS):
        total = total + weights[:, j : j + 1] * basis[j][:, pl.ds(mine, local)]
    solves[...] = root * total


def call(kernel, outs, scratch=()):
    return pl.pallas_call(
        kernel,
        out_shape=[jax.ShapeDtypeStruct(shape, dtype) for shape, dtype in outs],
        scratch_shapes=[pltpu.VMEM(shape, dtype) for shape, dtype in scratch],
        compiler_params=pltpu.CompilerParams(vmem_limit_bytes=16 * 2**20),
    )


def replicated(embeds, w_hidden, b_hidden, w_out, probes):
    count, local = probes.shape
    low, wide = jnp.bfloat16, jnp.float32
    block_own = gather_half(head(embeds, w_hidden, b_hidden, w_out, probes))
    half = block_own.shape[0] * local
    deep = w_out.shape[1] + LANES
    vector, square, table = ((count, half), wide), ((half, half), low), ((count, LANES), wide)
    block_oth = partner(block_own)
    kern_own, right, own = call(
        form_own_kernel, [square, ((half, deep), low), vector], [((half, deep), low)]
    )(block_own)
    kern_oth, oth, image = call(form_oth_kernel, [square, vector, vector], [((half, deep), low)])(
        block_oth, right, kern_own, own
    )
    basis, before = [own], ()
    for step in range(1, ITERS):
        after_own, after_oth, image, rates = call(
            functools.partial(step_kernel, step=step), [vector, vector, vector, table]
        )(*before, own, oth, image, partner(image), kern_own, kern_oth)
        before = (own, oth, rates)
        own, oth = after_own, after_oth
        basis.append(own)
    return call(
        finish_kernel,
        [((count, local), wide), ((count,), wide), ((count,), wide)],
        [((LANES, LANES), wide)],
    )(rates, oth, image, partner(image), *basis)


def rotate(matrix, vectors, first_idx, second_idx):
    diag_first = matrix[first_idx, first_idx]
    diag_second = matrix[second_idx, second_idx]
    off_value = matrix[first_idx, second_idx]
    half_angle = 0.5 * jnp.arctan2(2.0 * off_value, diag_first - diag_second)
    cosine = jnp.cos(half_angle)
    sine_val = jnp.sin(half_angle)
    row_first = matrix[first_idx]
    row_second = matrix[second_idx]
    matrix = matrix.at[first_idx].set(cosine * row_first + sine_val * row_second)
    matrix = matrix.at[second_idx].set(cosine * row_second - sine_val * row_first)
    col_first = matrix[:, first_idx]
    col_second = matrix[:, second_idx]
    matrix = matrix.at[:, first_idx].set(cosine * col_first + sine_val * col_second)
    matrix = matrix.at[:, second_idx].set(cosine * col_second - sine_val * col_first)
    vec_first = vectors[:, first_idx]
    vec_second = vectors[:, second_idx]
    vectors = vectors.at[:, first_idx].set(cosine * vec_first + sine_val * vec_second)
    vectors = vectors.at[:, second_idx].set(cosine * vec_second - sine_val * vec_first)
    return (matrix, vectors)


def quadrature(alphas, betas):
    tri_order = alphas.shape[0]
    identity = jnp.eye(tri_order, dtype=jnp.float32)
    upper_band = jnp.concatenate([jnp.zeros_like(alphas[:1]), betas], axis=0)
    shifted = jnp.eye(tri_order, k=1, dtype=jnp.float32)[:, :, None] * upper_band[None, :, :]
    matrix = identity[:, :, None] * alphas[None, :, :] + shifted + jnp.transpose(shifted, (1, 0, 2))
    vectors = jnp.broadcast_to(identity[:, :, None], matrix.shape)
    for sweep_index in range(SWEEPS):
        for first_idx in range(tri_order):
            for second_idx in range(first_idx + 1, tri_order):
                matrix, vectors = rotate(matrix, vectors, first_idx, second_idx)
    eigenvalues = jnp.maximum(jnp.sum(matrix * identity[:, :, None], axis=1), EIGEN_FLOOR)
    leading = vectors[0]
    logdet = jnp.sum(jnp.square(leading) * jnp.log(eigenvalues), axis=0)
    coefficients = jnp.sum(vectors * (leading / eigenvalues)[None, :, :], axis=1)
    scale_grad = 1.0 - NOISE_LEVEL * coefficients[0]
    return (logdet, scale_grad, coefficients)


def kernel_block(row_feats, row_norms, col_block, norm_block):
    inner = lax.dot_general(
        row_feats, col_block, (((1,), (1,)), ((), ())), preferred_element_type=jnp.float32
    )
    distance = row_norms[:, None] + norm_block[None, :] - 2.0 * inner
    return jnp.exp(-jnp.maximum(distance, 0.0) * INV_WIDTH).astype(jnp.bfloat16)


def block_width():
    return 512


def form_tile(row_feats, row_norms, col_feats, col_norms):
    total_cols = col_feats.shape[0]
    step_cols = block_width()
    block_count = total_cols // step_cols

    def one_block(block_index, tile):
        offset = block_index * step_cols
        col_block = lax.dynamic_slice_in_dim(col_feats, offset, step_cols, 0)
        norm_block = lax.dynamic_slice_in_dim(col_norms, offset, step_cols, 0)
        block = kernel_block(row_feats, row_norms, col_block, norm_block)
        return lax.dynamic_update_slice_in_dim(tile, block, offset, 1)

    empty = jnp.zeros((row_feats.shape[0], total_cols), jnp.bfloat16)
    return lax.fori_loop(0, block_count, one_block, empty)


def apply_kernel(vectors_low, tile):
    partial_value = lax.dot_general(
        lax.all_gather(vectors_low, "row", axis=1, tiled=True),
        tile,
        (((1,), (1,)), ((), ())),
        preferred_element_type=jnp.float32,
    )
    return lax.psum_scatter(partial_value, "grp", scatter_dimension=1, tiled=True)


def distributed(embeds, w_hidden, b_hidden, w_out, probes):
    hidden = jax.nn.gelu(
        jnp.dot(embeds, w_hidden, preferred_element_type=jnp.float32) + b_hidden
    ).astype(jnp.bfloat16)
    features = jnp.dot(hidden, w_out, preferred_element_type=jnp.float32).astype(jnp.bfloat16)
    row_feats = lax.all_gather(features, "grp", axis=0, tiled=True)
    col_feats = lax.all_gather(features, "row", axis=0, tiled=True)
    row_norms = jnp.sum(jnp.square(row_feats.astype(jnp.float32)), axis=1)
    col_norms = jnp.sum(jnp.square(col_feats.astype(jnp.float32)), axis=1)
    tile = form_tile(row_feats, row_norms, col_feats, col_norms)
    total_rows = probes.shape[1] * lax.axis_size("grp") * lax.axis_size("row")
    scale_root = math.sqrt(total_rows)
    current = (2 * probes - 1).astype(jnp.float32) / scale_root
    previous = jnp.zeros_like(current)
    beta_prev = jnp.zeros((current.shape[0],), jnp.float32)
    basis_list = []
    alpha_list = []
    beta_list = []
    for iteration in range(ITERS):
        kernel_image = apply_kernel(current.astype(jnp.bfloat16), tile) + NOISE_LEVEL * current
        moments = jnp.stack(
            [
                jnp.sum(current * kernel_image, axis=1),
                jnp.sum(kernel_image * kernel_image, axis=1),
                jnp.sum(previous * kernel_image, axis=1),
                jnp.sum(current * previous, axis=1),
                jnp.sum(current * current, axis=1),
                jnp.sum(previous * previous, axis=1),
            ]
        )
        moments = lax.psum(moments, ("grp", "row"))
        alpha_now = moments[0]
        residual_sq = (
            moments[1]
            + alpha_now * alpha_now * moments[4]
            + beta_prev * beta_prev * moments[5]
            - 2.0 * alpha_now * moments[0]
            - 2.0 * beta_prev * moments[2]
            + 2.0 * alpha_now * beta_prev * moments[3]
        )
        residual = kernel_image - alpha_now[:, None] * current - beta_prev[:, None] * previous
        basis_list.append(current)
        alpha_list.append(alpha_now)
        if iteration + 1 < ITERS:
            beta_now = jnp.sqrt(jnp.maximum(residual_sq, 0.0) + FLOOR_BETA)
            beta_list.append(beta_now)
            previous = current
            current = residual / beta_now[:, None]
            beta_prev = beta_now
    logdet, scale_grad, coefficients = quadrature(jnp.stack(alpha_list), jnp.stack(beta_list))
    solves = scale_root * jnp.einsum("jp,jpn->pn", coefficients, jnp.stack(basis_list))
    return (solves, logdet, scale_grad)


def power_of_two(value):
    return value & (value - 1) == 0


def solution(mesh):
    groups, lines = mesh.shape["grp"], mesh.shape["row"]

    def local(embeds, w_hidden, b_hidden, w_out, probes):
        rows = embeds.shape[0] * groups * lines
        fits = (
            rows * rows <= KERNEL_BYTES
            and lines % 2 == 0
            and power_of_two(groups)
            and power_of_two(lines)
            and probes.shape[1] == LANES
            and w_out.shape[1] == LANES
            and probes.shape[0] % 16 == 0
        )
        step = replicated if fits else distributed
        return step(embeds, w_hidden, b_hidden, w_out, probes)

    return jax.shard_map(
        local,
        mesh=mesh,
        in_specs=(P(("grp", "row"), None), P(), P(), P(), P(None, ("grp", "row"))),
        out_specs=(P(None, ("grp", "row")), P(), P()),
        check_vma=False,
    )
```

```python
import functools
import math

import jax
import jax.numpy as jnp
from jax import lax
from jax.experimental import pallas as pl
from jax.experimental.pallas import tpu as pltpu
from jax.sharding import PartitionSpec as P

ITERS = 8
SWEEPS = 6
INV_WIDTH = 1.0 / 12.0
NOISE_LEVEL = 0.5
FLOOR_BETA = 0.01
EIGEN_FLOOR = 0.25
LANES = 128
KERNEL_BYTES = 40 * 2**20


def head_kernel(embeds_ref, w_hidden_ref, b_hidden_ref, w_out_ref, probes_ref, out_ref):
    rows = embeds_ref.shape[0]
    hidden = jax.nn.gelu(
        jnp.dot(embeds_ref[...], w_hidden_ref[...], preferred_element_type=jnp.float32)
        + b_hidden_ref[...][None, :]
    ).astype(jnp.bfloat16)
    out_ref[:rows, :] = jnp.dot(
        hidden, w_out_ref[...], preferred_element_type=jnp.float32
    ).astype(jnp.bfloat16)
    out_ref[rows:, :] = probes_ref[...].astype(jnp.float32).astype(jnp.bfloat16)


def head(embeds, w_hidden, b_hidden, w_out, probes):
    rows, feat = embeds.shape[0], w_out.shape[1]
    return pl.pallas_call(
        head_kernel,
        out_shape=jax.ShapeDtypeStruct((rows + probes.shape[0], feat), jnp.bfloat16),
    )(embeds, w_hidden, b_hidden, w_out, probes)


def swap(value, axis, flip):
    size = lax.axis_size(axis)
    return lax.ppermute(value, axis, [(i, i ^ flip) for i in range(size)])


def gather_half(block):
    def spread(value, axis, stride):
        far = range(lax.axis_size(axis) // stride - 1, 0, -1)
        return jnp.concatenate([value] + [swap(value, axis, stride * k) for k in far][::-1])

    return spread(spread(block[None], "row", 2), "grp", 1)


def partner(value):
    return swap(value, "row", 1)


def pairs_of_round(order, turn):
    ring = order - 1
    pairs = [(ring, turn)]
    for gap in range(1, order // 2):
        pairs.append(((turn + gap) % ring, (turn - gap) % ring))
    return [tuple(sorted(pair)) for pair in pairs]


def jacobi_round(entries, columns, pairs):
    entries, columns = dict(entries), list(columns)

    def key(i, j):
        return (i, j) if i <= j else (j, i)

    turns = []
    for p, q in pairs:
        off = entries[p, q]
        gap = entries[q, q] - entries[p, p]
        root = jnp.abs(gap) + jnp.sqrt(gap * gap + 4.0 * off * off)
        numer = jnp.where(gap >= 0.0, 2.0 * off, -2.0 * off)
        tangent = jnp.where(root > 0.0, numer / jnp.where(root > 0.0, root, 1.0), 0.0)
        cosine = lax.rsqrt(1.0 + tangent * tangent)
        turns.append((cosine, cosine * tangent, tangent * off))
    for (p, q), (cosine, sine, shift) in zip(pairs, turns):
        entries[p, p] = entries[p, p] - shift
        entries[q, q] = entries[q, q] + shift
        entries[p, q] = jnp.zeros_like(shift)
        col_p, col_q = columns[p], columns[q]
        columns[p] = cosine * col_p - sine * col_q
        columns[q] = sine * col_p + cosine * col_q
    for a in range(len(pairs)):
        for b in range(a + 1, len(pairs)):
            (p, q), (r, s) = pairs[a], pairs[b]
            cos_a, sin_a, _ = turns[a]
            cos_b, sin_b, _ = turns[b]
            pr, ps = entries[key(p, r)], entries[key(p, s)]
            qr, qs = entries[key(q, r)], entries[key(q, s)]
            pr, qr = cos_a * pr - sin_a * qr, sin_a * pr + cos_a * qr
            ps, qs = cos_a * ps - sin_a * qs, sin_a * ps + cos_a * qs
            pr, ps = cos_b * pr - sin_b * ps, sin_b * pr + cos_b * ps
            qr, qs = cos_b * qr - sin_b * qs, sin_b * qr + cos_b * qs
            entries[key(p, r)], entries[key(p, s)] = pr, ps
            entries[key(q, r)], entries[key(q, s)] = qr, qs
    return entries, columns


def quadrature_lanes(alphas, betas, order):
    shape = alphas[0].shape
    keys = [(i, j) for i in range(order) for j in range(i, order)]
    entries = {}
    for i, j in keys:
        if i == j:
            entries[i, j] = alphas[i]
        elif j == i + 1:
            entries[i, j] = betas[i]
        else:
            entries[i, j] = jnp.zeros(shape, jnp.float32)
    sublane = lax.broadcasted_iota(jnp.int32, shape, 0)
    columns = [jnp.where(sublane == k, 1.0, 0.0).astype(jnp.float32) for k in range(order)]

    def sweep(_, state):
        values, columns = state
        entries = dict(zip(keys, values))
        for turn in range(order - 1):
            entries, columns = jacobi_round(entries, columns, pairs_of_round(order, turn))
        return tuple(entries[k] for k in keys), tuple(columns)

    values, columns = lax.fori_loop(
        0, SWEEPS, sweep, (tuple(entries[k] for k in keys), tuple(columns))
    )
    entries = dict(zip(keys, values))
    logdet = jnp.zeros((1, shape[1]), jnp.float32)
    coef = jnp.zeros(shape, jnp.float32)
    for k in range(order):
        eigen = jnp.maximum(entries[k, k][:1], EIGEN_FLOOR)
        leading = columns[k][:1]
        logdet = logdet + leading * leading * jnp.log(eigen)
        coef = coef + columns[k] * (leading / eigen)
    return logdet, coef


def split3(value):
    high = value.astype(jnp.bfloat16)
    rest = value - high.astype(jnp.float32)
    mid = rest.astype(jnp.bfloat16)
    low = (rest - mid.astype(jnp.float32)).astype(jnp.bfloat16)
    return high, mid, low


def slot_of(index):
    lines = lax.axis_size("row") // 2
    line, group = lax.axis_index("row") // 2, lax.axis_index("grp")
    return (group ^ (index // lines)) * lines + (line ^ (index % lines))


def place_blocks(blocks, left, right, start_vec, probes):
    count, block_rows, feat = blocks.shape
    local = block_rows - probes
    root = math.sqrt(2 * count * local)
    lane = lax.broadcasted_iota(jnp.int32, (local, LANES), 1)

    def extra(parts):
        total = jnp.zeros((local, LANES), jnp.float32)
        for k, part in enumerate(parts):
            total = jnp.where(lane == k, part, total)
        return total.astype(jnp.bfloat16)

    def place(index, carry):
        start = pl.multiple_of(slot_of(index) * local, local)
        feats = blocks[index, :local, :]
        wide = feats.astype(jnp.float32)
        norms = split3(-0.5 * jnp.sum(wide * wide, axis=1, keepdims=True))
        ones = (1.0, 1.0, 1.0)
        left[pl.ds(start, local), :feat] = feats
        left[pl.ds(start, local), feat:] = extra(norms + ones)
        if right is not None:
            right[pl.ds(start, local), :feat] = feats
            right[pl.ds(start, local), feat:] = extra(ones + norms)
        bits = blocks[index, local:, :].astype(jnp.float32)
        start_vec[:, pl.ds(start, local)] = (2.0 * bits - 1.0) / root
        return carry

    lax.fori_loop(0, count, place, 0, unroll=4)


def form(left, right, kern):
    rows, cols = left.shape[0], right.shape[0]
    width, height = 512, 512

    def columns(step, carry):
        start = pl.multiple_of(step * width, width)
        block = right[pl.ds(start, width), :]
        for top in range(0, rows, height):
            inner = lax.dot_general(
                left[top : top + height, :],
                block,
                (((1,), (1,)), ((), ())),
                preferred_element_type=jnp.float32,
            )
            kern[top : top + height, pl.ds(start, width)] = jnp.exp2(
                jnp.minimum(inner, 0.0) * (2.0 * INV_WIDTH * math.log2(math.e))
            ).astype(jnp.bfloat16)
        return carry

    lax.fori_loop(0, cols // width, columns, 0)


def product(vectors, kern):
    count = vectors[0].shape[0]
    pieces = jnp.concatenate([piece for vector in vectors for piece in split3(vector)])
    width = 512
    parts = [[] for _ in vectors]
    for start in range(0, kern.shape[1], width):
        whole = jnp.dot(
            pieces, kern[:, start : start + width], preferred_element_type=jnp.float32
        )
        for k, part in enumerate(parts):
            high, mid, low = (
                whole[(3 * k + i) * count : (3 * k + i + 1) * count] for i in range(3)
            )
            part.append(high + (mid + low))
    return [jnp.concatenate(part, axis=1) for part in parts]


def form_own_kernel(blocks, kern, right, start_vec, left):
    place_blocks(blocks, left, right, start_vec, start_vec.shape[0])
    form(left, right, kern)


def form_oth_kernel(blocks, right, kern_own, own_vec, kern, start_vec, image, left):
    place_blocks(blocks, left, None, start_vec, start_vec.shape[0])
    form(left, right, kern)
    image[...] = product([own_vec[...]], kern_own)[0] + product([start_vec[...]], kern)[0]


def row_sum(first, second):
    return jnp.sum(first * second, axis=1, keepdims=True)


def ahead_kernel(*refs, step):
    if step > 1:
        before_own, table, *refs = refs
    own, image_own, kern_own, ahead, along = refs
    q_own = own[...]
    w_own = image_own[...] + NOISE_LEVEL * q_own
    if step > 1:
        w_own = w_own - table[:, ITERS + step - 2 : ITERS + step - 1] * before_own[...]
    ahead[...], along[...] = product([w_own, q_own], kern_own)


def step_kernel(*refs, step):
    if step > 1:
        before_own, before_oth, table, *refs = refs
    own, oth, image_own, image_oth, ahead, along, kern_oth, *outs = refs
    next_own, next_oth, image, table_out = outs
    lane = lax.broadcasted_iota(jnp.int32, table_out.shape, 1)
    q_own, q_oth = own[...], oth[...]
    w_own = image_own[...] + NOISE_LEVEL * q_own
    w_oth = image_oth[...] + NOISE_LEVEL * q_oth
    alpha = row_sum(q_own, w_own) + row_sum(q_oth, w_oth)
    w_own = w_own - alpha * q_own
    w_oth = w_oth - alpha * q_oth
    if step > 1:
        last = table[...]
        beta = last[:, ITERS + step - 2 : ITERS + step - 1]
        w_own = w_own - beta * before_own[...]
        w_oth = w_oth - beta * before_oth[...]
    else:
        last = jnp.zeros(table_out.shape, jnp.float32)
    beta = jnp.sqrt(
        jnp.maximum(row_sum(w_own, w_own) + row_sum(w_oth, w_oth), 0.0) + FLOOR_BETA
    )
    w_own, w_oth = w_own / beta, w_oth / beta
    next_own[...], next_oth[...] = w_own, w_oth
    table_out[...] = jnp.where(
        lane == step - 1, alpha, jnp.where(lane == ITERS + step - 1, beta, last)
    )
    image[...] = (ahead[...] - alpha * along[...]) / beta + product([w_oth], kern_oth)[0]


def finish_kernel(*refs):
    table, oth, image_own, image_oth, *basis = refs[: 4 + ITERS]
    solves, logdet_ref, scale_ref, square = refs[4 + ITERS :]
    probes, local = solves.shape
    root = math.sqrt(2 * oth.shape[1])
    own = basis[-1]
    alpha = row_sum(own[...], image_own[...] + NOISE_LEVEL * own[...]) + row_sum(
        oth[...], image_oth[...] + NOISE_LEVEL * oth[...]
    )
    lane = lax.broadcasted_iota(jnp.int32, table.shape, 1)
    square[...] = jnp.zeros_like(square)
    square[:probes, :] = jnp.where(lane == ITERS - 1, alpha, table[...])
    turned = jnp.transpose(square[...])
    spread = lambda j: jnp.broadcast_to(turned[j : j + 1, :], (8, LANES))
    logdet, coef = quadrature_lanes(
        [spread(j) for j in range(ITERS)], [spread(ITERS + j) for j in range(ITERS - 1)], ITERS
    )
    logdet_ref[...] = logdet[0, :probes]
    scale_ref[...] = 1.0 - NOISE_LEVEL * coef[0, :probes]
    square[:ITERS, :] = coef
    weights = jnp.transpose(square[...])[:probes, :]
    mine = pl.multiple_of(slot_of(0) * local, local)
    total = jnp.zeros((probes, local), jnp.float32)
    for j in range(ITERS):
        total = total + weights[:, j : j + 1] * basis[j][:, pl.ds(mine, local)]
    solves[...] = root * total


def call(kernel, outs, scratch=()):
    return pl.pallas_call(
        kernel,
        out_shape=[jax.ShapeDtypeStruct(shape, dtype) for shape, dtype in outs],
        scratch_shapes=[pltpu.VMEM(shape, dtype) for shape, dtype in scratch],
        compiler_params=pltpu.CompilerParams(vmem_limit_bytes=16 * 2**20),
    )


def replicated(embeds, w_hidden, b_hidden, w_out, probes):
    count, local = probes.shape
    low, wide = jnp.bfloat16, jnp.float32
    block_own = gather_half(head(embeds, w_hidden, b_hidden, w_out, probes))
    half = block_own.shape[0] * local
    deep = w_out.shape[1] + LANES
    vector, square, table = ((count, half), wide), ((half, half), low), ((count, LANES), wide)
    block_oth = partner(block_own)
    kern_own, right, own = call(
        form_own_kernel, [square, ((half, deep), low), vector], [((half, deep), low)]
    )(block_own)
    kern_oth, oth, image = call(form_oth_kernel, [square, vector, vector], [((half, deep), low)])(
        block_oth, right, kern_own, own
    )
    basis, before = [own], ()
    for step in range(1, ITERS):
        image_oth = partner(image)
        ahead, along = call(functools.partial(ahead_kernel, step=step), [vector, vector])(
            *before[::2], own, image, kern_own
        )
        after_own, after_oth, image, rates = call(
            functools.partial(step_kernel, step=step), [vector, vector, vector, table]
        )(*before, own, oth, image, image_oth, ahead, along, kern_oth)
        before = (own, oth, rates)
        own, oth = after_own, after_oth
        basis.append(own)
    return call(
        finish_kernel,
        [((count, local), wide), ((count,), wide), ((count,), wide)],
        [((LANES, LANES), wide)],
    )(rates, oth, image, partner(image), *basis)


def rotate(matrix, vectors, first_idx, second_idx):
    diag_first = matrix[first_idx, first_idx]
    diag_second = matrix[second_idx, second_idx]
    off_value = matrix[first_idx, second_idx]
    half_angle = 0.5 * jnp.arctan2(2.0 * off_value, diag_first - diag_second)
    cosine = jnp.cos(half_angle)
    sine_val = jnp.sin(half_angle)
    row_first = matrix[first_idx]
    row_second = matrix[second_idx]
    matrix = matrix.at[first_idx].set(cosine * row_first + sine_val * row_second)
    matrix = matrix.at[second_idx].set(cosine * row_second - sine_val * row_first)
    col_first = matrix[:, first_idx]
    col_second = matrix[:, second_idx]
    matrix = matrix.at[:, first_idx].set(cosine * col_first + sine_val * col_second)
    matrix = matrix.at[:, second_idx].set(cosine * col_second - sine_val * col_first)
    vec_first = vectors[:, first_idx]
    vec_second = vectors[:, second_idx]
    vectors = vectors.at[:, first_idx].set(cosine * vec_first + sine_val * vec_second)
    vectors = vectors.at[:, second_idx].set(cosine * vec_second - sine_val * vec_first)
    return (matrix, vectors)


def quadrature(alphas, betas):
    tri_order = alphas.shape[0]
    identity = jnp.eye(tri_order, dtype=jnp.float32)
    upper_band = jnp.concatenate([jnp.zeros_like(alphas[:1]), betas], axis=0)
    shifted = jnp.eye(tri_order, k=1, dtype=jnp.float32)[:, :, None] * upper_band[None, :, :]
    matrix = identity[:, :, None] * alphas[None, :, :] + shifted + jnp.transpose(shifted, (1, 0, 2))
    vectors = jnp.broadcast_to(identity[:, :, None], matrix.shape)
    for sweep_index in range(SWEEPS):
        for first_idx in range(tri_order):
            for second_idx in range(first_idx + 1, tri_order):
                matrix, vectors = rotate(matrix, vectors, first_idx, second_idx)
    eigenvalues = jnp.maximum(jnp.sum(matrix * identity[:, :, None], axis=1), EIGEN_FLOOR)
    leading = vectors[0]
    logdet = jnp.sum(jnp.square(leading) * jnp.log(eigenvalues), axis=0)
    coefficients = jnp.sum(vectors * (leading / eigenvalues)[None, :, :], axis=1)
    scale_grad = 1.0 - NOISE_LEVEL * coefficients[0]
    return (logdet, scale_grad, coefficients)


def kernel_block(row_feats, row_norms, col_block, norm_block):
    inner = lax.dot_general(
        row_feats, col_block, (((1,), (1,)), ((), ())), preferred_element_type=jnp.float32
    )
    distance = row_norms[:, None] + norm_block[None, :] - 2.0 * inner
    return jnp.exp(-jnp.maximum(distance, 0.0) * INV_WIDTH).astype(jnp.bfloat16)


def block_width():
    return 512


def form_tile(row_feats, row_norms, col_feats, col_norms):
    total_cols = col_feats.shape[0]
    step_cols = block_width()
    block_count = total_cols // step_cols

    def one_block(block_index, tile):
        offset = block_index * step_cols
        col_block = lax.dynamic_slice_in_dim(col_feats, offset, step_cols, 0)
        norm_block = lax.dynamic_slice_in_dim(col_norms, offset, step_cols, 0)
        block = kernel_block(row_feats, row_norms, col_block, norm_block)
        return lax.dynamic_update_slice_in_dim(tile, block, offset, 1)

    empty = jnp.zeros((row_feats.shape[0], total_cols), jnp.bfloat16)
    return lax.fori_loop(0, block_count, one_block, empty)


def apply_kernel(vectors_low, tile):
    partial_value = lax.dot_general(
        lax.all_gather(vectors_low, "row", axis=1, tiled=True),
        tile,
        (((1,), (1,)), ((), ())),
        preferred_element_type=jnp.float32,
    )
    return lax.psum_scatter(partial_value, "grp", scatter_dimension=1, tiled=True)


def distributed(embeds, w_hidden, b_hidden, w_out, probes):
    hidden = jax.nn.gelu(
        jnp.dot(embeds, w_hidden, preferred_element_type=jnp.float32) + b_hidden
    ).astype(jnp.bfloat16)
    features = jnp.dot(hidden, w_out, preferred_element_type=jnp.float32).astype(jnp.bfloat16)
    row_feats = lax.all_gather(features, "grp", axis=0, tiled=True)
    col_feats = lax.all_gather(features, "row", axis=0, tiled=True)
    row_norms = jnp.sum(jnp.square(row_feats.astype(jnp.float32)), axis=1)
    col_norms = jnp.sum(jnp.square(col_feats.astype(jnp.float32)), axis=1)
    tile = form_tile(row_feats, row_norms, col_feats, col_norms)
    total_rows = probes.shape[1] * lax.axis_size("grp") * lax.axis_size("row")
    scale_root = math.sqrt(total_rows)
    current = (2 * probes - 1).astype(jnp.float32) / scale_root
    previous = jnp.zeros_like(current)
    beta_prev = jnp.zeros((current.shape[0],), jnp.float32)
    basis_list = []
    alpha_list = []
    beta_list = []
    for iteration in range(ITERS):
        kernel_image = apply_kernel(current.astype(jnp.bfloat16), tile) + NOISE_LEVEL * current
        moments = jnp.stack(
            [
                jnp.sum(current * kernel_image, axis=1),
                jnp.sum(kernel_image * kernel_image, axis=1),
                jnp.sum(previous * kernel_image, axis=1),
                jnp.sum(current * previous, axis=1),
                jnp.sum(current * current, axis=1),
                jnp.sum(previous * previous, axis=1),
            ]
        )
        moments = lax.psum(moments, ("grp", "row"))
        alpha_now = moments[0]
        residual_sq = (
            moments[1]
            + alpha_now * alpha_now * moments[4]
            + beta_prev * beta_prev * moments[5]
            - 2.0 * alpha_now * moments[0]
            - 2.0 * beta_prev * moments[2]
            + 2.0 * alpha_now * beta_prev * moments[3]
        )
        residual = kernel_image - alpha_now[:, None] * current - beta_prev[:, None] * previous
        basis_list.append(current)
        alpha_list.append(alpha_now)
        if iteration + 1 < ITERS:
            beta_now = jnp.sqrt(jnp.maximum(residual_sq, 0.0) + FLOOR_BETA)
            beta_list.append(beta_now)
            previous = current
            current = residual / beta_now[:, None]
            beta_prev = beta_now
    logdet, scale_grad, coefficients = quadrature(jnp.stack(alpha_list), jnp.stack(beta_list))
    solves = scale_root * jnp.einsum("jp,jpn->pn", coefficients, jnp.stack(basis_list))
    return (solves, logdet, scale_grad)


def power_of_two(value):
    return value & (value - 1) == 0


def solution(mesh):
    groups, lines = mesh.shape["grp"], mesh.shape["row"]

    def local(embeds, w_hidden, b_hidden, w_out, probes):
        rows = embeds.shape[0] * groups * lines
        fits = (
            rows * rows <= KERNEL_BYTES
            and lines % 2 == 0
            and power_of_two(groups)
            and power_of_two(lines)
            and probes.shape[1] == LANES
            and w_out.shape[1] == LANES
            and probes.shape[0] % 16 == 0
        )
        step = replicated if fits else distributed
        return step(embeds, w_hidden, b_hidden, w_out, probes)

    return jax.shard_map(
        local,
        mesh=mesh,
        in_specs=(P(("grp", "row"), None), P(), P(), P(), P(None, ("grp", "row"))),
        out_specs=(P(None, ("grp", "row")), P(), P()),
        check_vma=False,
    )
```

```python
import functools
import math

import jax
import jax.numpy as jnp
from jax import lax
from jax.experimental import pallas as pl
from jax.experimental.pallas import tpu as pltpu
from jax.sharding import PartitionSpec as P

ITERS = 8
SWEEPS = 6
INV_WIDTH = 1.0 / 12.0
NOISE_LEVEL = 0.5
FLOOR_BETA = 0.01
EIGEN_FLOOR = 0.25
LANES = 128
TINY = 1e-30
KERNEL_BYTES = 40 * 2**20


def head_kernel(*refs):
    sources, (out_ref, *places, sems) = refs[:5], refs[5:]
    copies = [
        pltpu.make_async_copy(source, place, sems.at[k])
        for k, (source, place) in enumerate(zip(sources, places))
    ]
    for copy in copies:
        copy.start()
    embeds, w_hidden, b_hidden, w_out, probes = places
    rows = embeds.shape[0]
    for copy in copies:
        copy.wait()
    hidden = jax.nn.gelu(
        jnp.dot(embeds[...], w_hidden[...], preferred_element_type=jnp.float32)
        + b_hidden[...][None, :]
    ).astype(jnp.bfloat16)
    out_ref[:rows, :] = jnp.dot(
        hidden, w_out[...], preferred_element_type=jnp.float32
    ).astype(jnp.bfloat16)
    out_ref[rows:, :] = probes[...].astype(jnp.float32).astype(jnp.bfloat16)


def head(*arrays):
    embeds, w_out, probes = arrays[0], arrays[3], arrays[4]
    shape = (embeds.shape[0] + probes.shape[0], w_out.shape[1])
    return pl.pallas_call(
        head_kernel,
        out_shape=pltpu.VMEM(shape, jnp.bfloat16),
        in_specs=[pl.BlockSpec(memory_space=pl.ANY)] * len(arrays),
        out_specs=pl.BlockSpec(memory_space=pltpu.VMEM),
        scratch_shapes=[pltpu.VMEM(a.shape, a.dtype) for a in arrays]
        + [pltpu.SemaphoreType.DMA((len(arrays),))],
    )(*arrays)


def swap(value, axis, flip):
    size = lax.axis_size(axis)
    return lax.ppermute(value, axis, [(i, i ^ flip) for i in range(size)])


def gather_half(block):
    def spread(value, axis, stride):
        far = range(1, lax.axis_size(axis) // stride)
        return jnp.concatenate([value] + [swap(value, axis, stride * k) for k in far])

    return spread(spread(block[None], "row", 2), "grp", 1)


def partner(value):
    return swap(value, "row", 1)


def pairs_of_round(order, turn):
    ring = order - 1
    pairs = [(ring, turn)]
    for gap in range(1, order // 2):
        pairs.append(((turn + gap) % ring, (turn - gap) % ring))
    return [tuple(sorted(pair)) for pair in pairs]


def jacobi_round(entries, columns, pairs):
    entries, columns = dict(entries), list(columns)

    def key(i, j):
        return (i, j) if i <= j else (j, i)

    turns = []
    for p, q in pairs:
        double = 2.0 * entries[p, q]
        gap = entries[q, q] - entries[p, p]
        square = gap * gap + double * double
        live = square > TINY
        inverse = lax.rsqrt(jnp.where(live, square, 1.0))
        width = jnp.where(live, square * inverse, 0.0)
        cos_square = jnp.where(live, 0.5 + 0.5 * jnp.abs(gap) * inverse, 1.0)
        sine_half = jnp.where(live, 0.5 * double * inverse, 0.0)
        upward = gap >= 0.0
        secant = lax.rsqrt(cos_square)
        cosine = cos_square * secant
        sine = jnp.where(upward, sine_half, -sine_half) * secant
        turns.append((cosine, sine, jnp.where(upward, width, -width)))
    for (p, q), (cosine, sine, width) in zip(pairs, turns):
        middle = entries[p, p] + entries[q, q]
        entries[p, p] = 0.5 * (middle - width)
        entries[q, q] = 0.5 * (middle + width)
        entries[p, q] = jnp.zeros_like(width)
        col_p, col_q = columns[p], columns[q]
        columns[p] = cosine * col_p - sine * col_q
        columns[q] = sine * col_p + cosine * col_q
    for a in range(len(pairs)):
        for b in range(a + 1, len(pairs)):
            (p, q), (r, s) = pairs[a], pairs[b]
            cos_a, sin_a, _ = turns[a]
            cos_b, sin_b, _ = turns[b]
            pr, ps = entries[key(p, r)], entries[key(p, s)]
            qr, qs = entries[key(q, r)], entries[key(q, s)]
            pr, qr = cos_a * pr - sin_a * qr, sin_a * pr + cos_a * qr
            ps, qs = cos_a * ps - sin_a * qs, sin_a * ps + cos_a * qs
            pr, ps = cos_b * pr - sin_b * ps, sin_b * pr + cos_b * ps
            qr, qs = cos_b * qr - sin_b * qs, sin_b * qr + cos_b * qs
            entries[key(p, r)], entries[key(p, s)] = pr, ps
            entries[key(q, r)], entries[key(q, s)] = qr, qs
    return entries, columns


def quadrature_lanes(alphas, betas, order):
    shape = alphas[0].shape
    keys = [(i, j) for i in range(order) for j in range(i, order)]
    entries = {}
    for i, j in keys:
        if i == j:
            entries[i, j] = alphas[i]
        elif j == i + 1:
            entries[i, j] = betas[i]
        else:
            entries[i, j] = jnp.zeros(shape, jnp.float32)
    sublane = lax.broadcasted_iota(jnp.int32, shape, 0)
    columns = [jnp.where(sublane == k, 1.0, 0.0).astype(jnp.float32) for k in range(order)]

    def sweep(_, state):
        values, columns = state
        entries = dict(zip(keys, values))
        for turn in range(order - 1):
            entries, columns = jacobi_round(entries, columns, pairs_of_round(order, turn))
        return tuple(entries[k] for k in keys), tuple(columns)

    values, columns = lax.fori_loop(
        0, SWEEPS, sweep, (tuple(entries[k] for k in keys), tuple(columns))
    )
    entries = dict(zip(keys, values))
    logdet = jnp.zeros((1, shape[1]), jnp.float32)
    coef = jnp.zeros(shape, jnp.float32)
    for k in range(order):
        eigen = jnp.maximum(entries[k, k][:1], EIGEN_FLOOR)
        leading = columns[k][:1]
        logdet = logdet + leading * leading * jnp.log(eigen)
        coef = coef + columns[k] * (leading / eigen)
    return logdet, coef


def split3(value):
    high = value.astype(jnp.bfloat16)
    rest = value - high.astype(jnp.float32)
    mid = rest.astype(jnp.bfloat16)
    low = (rest - mid.astype(jnp.float32)).astype(jnp.bfloat16)
    return high, mid, low


def slot_of(index):
    lines = lax.axis_size("row") // 2
    line, group = lax.axis_index("row") // 2, lax.axis_index("grp")
    return (group ^ (index // lines)) * lines + (line ^ (index % lines))


def place_kernel(blocks, left, right, start_vec):
    count, block_rows, feat = blocks.shape
    local = block_rows - start_vec.shape[0]
    root = math.sqrt(2 * count * local)
    lane = lax.broadcasted_iota(jnp.int32, (local, LANES), 1)
    adder = jnp.ones((2 * feat, LANES), jnp.bfloat16)

    def extra(parts, first, ones):
        total = jnp.where((lane >= ones) & (lane < ones + 3), 1.0, 0.0)
        for k, part in enumerate(parts):
            total = jnp.where(lane == first + k, part.astype(jnp.float32), total)
        return total.astype(jnp.bfloat16)

    def place(index, carry):
        start = pl.multiple_of(slot_of(index) * local, local)
        feats = blocks[index, :local, :]
        wide = feats.astype(jnp.float32)
        square = wide * wide
        high = square.astype(jnp.bfloat16)
        low = (square - high.astype(jnp.float32)).astype(jnp.bfloat16)
        total = jnp.dot(
            jnp.concatenate([high, low], axis=1), adder, preferred_element_type=jnp.float32
        )
        norms = split3(-0.5 * total)
        left[pl.ds(start, local), :feat] = feats
        left[pl.ds(start, local), feat:] = extra(norms, 0, 3)
        right[pl.ds(start, local), :feat] = feats
        right[pl.ds(start, local), feat:] = extra(norms, 3, 0)
        bits = blocks[index, local:, :].astype(jnp.float32)
        start_vec[:, pl.ds(start, local)] = (2.0 * bits - 1.0) / root
        return carry

    lax.fori_loop(0, count, place, 0, unroll=8)


def form(left, right, kern):
    width, height = 512, 512
    for start in range(0, right.shape[0], width):
        block = right[start : start + width, :]
        for top in range(0, left.shape[0], height):
            inner = lax.dot_general(
                left[top : top + height, :],
                block,
                (((1,), (1,)), ((), ())),
                preferred_element_type=jnp.float32,
            )
            kern[top : top + height, start : start + width] = jnp.exp2(
                jnp.minimum(inner, 0.0) * (2.0 * INV_WIDTH * math.log2(math.e))
            ).astype(jnp.bfloat16)


def product(vectors, kern):
    count = vectors[0].shape[0]
    pieces = jnp.concatenate([piece for vector in vectors for piece in split3(vector)])
    width = 512
    parts = [[] for _ in vectors]
    for start in range(0, kern.shape[1], width):
        whole = jnp.dot(
            pieces, kern[:, start : start + width], preferred_element_type=jnp.float32
        )
        for k, part in enumerate(parts):
            high, mid, low = (
                whole[(3 * k + i) * count : (3 * k + i + 1) * count] for i in range(3)
            )
            part.append(high + (mid + low))
    return [jnp.concatenate(part, axis=1) for part in parts]


def form_own_kernel(left, right, kern):
    form(left, right, kern)


def form_oth_kernel(left, right, kern_own, own, oth, kern, image):
    form(left, right, kern)
    image[...] = product([own[...]], kern_own)[0] + product([oth[...]], kern)[0]


def row_sum(first, second):
    return jnp.sum(first * second, axis=1, keepdims=True)


def ahead_kernel(*refs, step):
    if step > 1:
        before_own, table, *refs = refs
    own, image_own, kern_own, ahead, along = refs
    q_own = own[...]
    u_own = image_own[...] + NOISE_LEVEL * q_own
    if step > 1:
        u_own = u_own - table[:, ITERS + step - 2 : ITERS + step - 1] * before_own[...]
    ahead[...], along[...] = product([u_own, q_own], kern_own)


def step_kernel(*refs, step):
    if step > 1:
        before_own, before_oth, table, *refs = refs
    own, oth, image_own, image_oth, ahead, along, kern_oth, *outs = refs
    next_own, next_oth, image, table_out = outs
    lane = lax.broadcasted_iota(jnp.int32, table_out.shape, 1)
    q_own, q_oth = own[...], oth[...]
    w_own = image_own[...] + NOISE_LEVEL * q_own
    w_oth = image_oth[...] + NOISE_LEVEL * q_oth
    u_own, u_oth, last = w_own, w_oth, jnp.zeros(table_out.shape, jnp.float32)
    if step > 1:
        last = table[...]
        beta = last[:, ITERS + step - 2 : ITERS + step - 1]
        u_own = u_own - beta * before_own[...]
        u_oth = u_oth - beta * before_oth[...]
    ahead_oth, along_oth = product([u_oth, q_oth], kern_oth)
    alpha = row_sum(q_own, w_own) + row_sum(q_oth, w_oth)
    r_own, r_oth = u_own - alpha * q_own, u_oth - alpha * q_oth
    beta = jnp.sqrt(
        jnp.maximum(row_sum(r_own, r_own) + row_sum(r_oth, r_oth), 0.0) + FLOOR_BETA
    )
    next_own[...], next_oth[...] = r_own / beta, r_oth / beta
    table_out[...] = jnp.where(
        lane == step - 1, alpha, jnp.where(lane == ITERS + step - 1, beta, last)
    )
    image[...] = (ahead[...] + ahead_oth - alpha * (along[...] + along_oth)) / beta


def finish_kernel(*refs):
    table, oth, image_own, image_oth, *basis = refs[: 4 + ITERS]
    solves, logdet_ref, scale_ref, square = refs[4 + ITERS :]
    probes, local = solves.shape
    root = math.sqrt(2 * oth.shape[1])
    own = basis[-1]
    alpha = row_sum(own[...], image_own[...] + NOISE_LEVEL * own[...]) + row_sum(
        oth[...], image_oth[...] + NOISE_LEVEL * oth[...]
    )
    lane = lax.broadcasted_iota(jnp.int32, table.shape, 1)
    square[...] = jnp.zeros_like(square)
    square[:probes, :] = jnp.where(lane == ITERS - 1, alpha, table[...])
    turned = jnp.transpose(square[...])
    spread = lambda j: jnp.broadcast_to(turned[j : j + 1, :], (8, LANES))
    logdet, coef = quadrature_lanes(
        [spread(j) for j in range(ITERS)], [spread(ITERS + j) for j in range(ITERS - 1)], ITERS
    )
    logdet_ref[...] = logdet[0, :probes]
    scale_ref[...] = 1.0 - NOISE_LEVEL * coef[0, :probes]
    square[:ITERS, :] = coef
    weights = jnp.transpose(square[...])[:probes, :]
    mine = pl.multiple_of(slot_of(0) * local, local)
    total = jnp.zeros((probes, local), jnp.float32)
    for j in range(ITERS):
        total = total + weights[:, j : j + 1] * basis[j][:, pl.ds(mine, local)]
    solves[...] = root * total


def call(kernel, outs, scratch=()):
    return pl.pallas_call(
        kernel,
        out_shape=[jax.ShapeDtypeStruct(shape, dtype) for shape, dtype in outs],
        scratch_shapes=[pltpu.VMEM(shape, dtype) for shape, dtype in scratch],
        compiler_params=pltpu.CompilerParams(vmem_limit_bytes=16 * 2**20),
    )


def replicated(embeds, w_hidden, b_hidden, w_out, probes):
    count, local = probes.shape
    low, wide = jnp.bfloat16, jnp.float32
    block_own = gather_half(head(embeds, w_hidden, b_hidden, w_out, probes))
    half = block_own.shape[0] * local
    deep = w_out.shape[1] + LANES
    vector, square, table = ((count, half), wide), ((half, half), low), ((count, LANES), wide)
    features = ((half, deep), low)
    left, right, own = call(place_kernel, [features, features, vector])(block_own)
    left_oth, oth = partner(left), partner(own)
    (kern_own,) = call(form_own_kernel, [square])(left, right)
    kern_oth, image = call(form_oth_kernel, [square, vector])(
        left_oth, right, kern_own, own, oth
    )
    basis, before = [own], ()
    for step in range(1, ITERS):
        image_oth = partner(image)
        ahead, along = call(functools.partial(ahead_kernel, step=step), [vector, vector])(
            *before[::2], own, image, kern_own
        )
        after_own, after_oth, image, rates = call(
            functools.partial(step_kernel, step=step), [vector, vector, vector, table]
        )(*before, own, oth, image, image_oth, ahead, along, kern_oth)
        before = (own, oth, rates)
        own, oth = after_own, after_oth
        basis.append(own)
    return call(
        finish_kernel,
        [((count, local), wide), ((count,), wide), ((count,), wide)],
        [((LANES, LANES), wide)],
    )(rates, oth, image, partner(image), *basis)


def rotate(matrix, vectors, first_idx, second_idx):
    diag_first = matrix[first_idx, first_idx]
    diag_second = matrix[second_idx, second_idx]
    off_value = matrix[first_idx, second_idx]
    half_angle = 0.5 * jnp.arctan2(2.0 * off_value, diag_first - diag_second)
    cosine = jnp.cos(half_angle)
    sine_val = jnp.sin(half_angle)
    row_first = matrix[first_idx]
    row_second = matrix[second_idx]
    matrix = matrix.at[first_idx].set(cosine * row_first + sine_val * row_second)
    matrix = matrix.at[second_idx].set(cosine * row_second - sine_val * row_first)
    col_first = matrix[:, first_idx]
    col_second = matrix[:, second_idx]
    matrix = matrix.at[:, first_idx].set(cosine * col_first + sine_val * col_second)
    matrix = matrix.at[:, second_idx].set(cosine * col_second - sine_val * col_first)
    vec_first = vectors[:, first_idx]
    vec_second = vectors[:, second_idx]
    vectors = vectors.at[:, first_idx].set(cosine * vec_first + sine_val * vec_second)
    vectors = vectors.at[:, second_idx].set(cosine * vec_second - sine_val * vec_first)
    return (matrix, vectors)


def quadrature(alphas, betas):
    tri_order = alphas.shape[0]
    identity = jnp.eye(tri_order, dtype=jnp.float32)
    upper_band = jnp.concatenate([jnp.zeros_like(alphas[:1]), betas], axis=0)
    shifted = jnp.eye(tri_order, k=1, dtype=jnp.float32)[:, :, None] * upper_band[None, :, :]
    matrix = identity[:, :, None] * alphas[None, :, :] + shifted + jnp.transpose(shifted, (1, 0, 2))
    vectors = jnp.broadcast_to(identity[:, :, None], matrix.shape)
    for sweep_index in range(SWEEPS):
        for first_idx in range(tri_order):
            for second_idx in range(first_idx + 1, tri_order):
                matrix, vectors = rotate(matrix, vectors, first_idx, second_idx)
    eigenvalues = jnp.maximum(jnp.sum(matrix * identity[:, :, None], axis=1), EIGEN_FLOOR)
    leading = vectors[0]
    logdet = jnp.sum(jnp.square(leading) * jnp.log(eigenvalues), axis=0)
    coefficients = jnp.sum(vectors * (leading / eigenvalues)[None, :, :], axis=1)
    scale_grad = 1.0 - NOISE_LEVEL * coefficients[0]
    return (logdet, scale_grad, coefficients)


def kernel_block(row_feats, row_norms, col_block, norm_block):
    inner = lax.dot_general(
        row_feats, col_block, (((1,), (1,)), ((), ())), preferred_element_type=jnp.float32
    )
    distance = row_norms[:, None] + norm_block[None, :] - 2.0 * inner
    return jnp.exp(-jnp.maximum(distance, 0.0) * INV_WIDTH).astype(jnp.bfloat16)


def block_width():
    return 512


def form_tile(row_feats, row_norms, col_feats, col_norms):
    total_cols = col_feats.shape[0]
    step_cols = block_width()
    block_count = total_cols // step_cols

    def one_block(block_index, tile):
        offset = block_index * step_cols
        col_block = lax.dynamic_slice_in_dim(col_feats, offset, step_cols, 0)
        norm_block = lax.dynamic_slice_in_dim(col_norms, offset, step_cols, 0)
        block = kernel_block(row_feats, row_norms, col_block, norm_block)
        return lax.dynamic_update_slice_in_dim(tile, block, offset, 1)

    empty = jnp.zeros((row_feats.shape[0], total_cols), jnp.bfloat16)
    return lax.fori_loop(0, block_count, one_block, empty)


def apply_kernel(vectors_low, tile):
    partial_value = lax.dot_general(
        lax.all_gather(vectors_low, "row", axis=1, tiled=True),
        tile,
        (((1,), (1,)), ((), ())),
        preferred_element_type=jnp.float32,
    )
    return lax.psum_scatter(partial_value, "grp", scatter_dimension=1, tiled=True)


def distributed(embeds, w_hidden, b_hidden, w_out, probes):
    hidden = jax.nn.gelu(
        jnp.dot(embeds, w_hidden, preferred_element_type=jnp.float32) + b_hidden
    ).astype(jnp.bfloat16)
    features = jnp.dot(hidden, w_out, preferred_element_type=jnp.float32).astype(jnp.bfloat16)
    row_feats = lax.all_gather(features, "grp", axis=0, tiled=True)
    col_feats = lax.all_gather(features, "row", axis=0, tiled=True)
    row_norms = jnp.sum(jnp.square(row_feats.astype(jnp.float32)), axis=1)
    col_norms = jnp.sum(jnp.square(col_feats.astype(jnp.float32)), axis=1)
    tile = form_tile(row_feats, row_norms, col_feats, col_norms)
    total_rows = probes.shape[1] * lax.axis_size("grp") * lax.axis_size("row")
    scale_root = math.sqrt(total_rows)
    current = (2 * probes - 1).astype(jnp.float32) / scale_root
    previous = jnp.zeros_like(current)
    beta_prev = jnp.zeros((current.shape[0],), jnp.float32)
    basis_list = []
    alpha_list = []
    beta_list = []
    for iteration in range(ITERS):
        kernel_image = apply_kernel(current.astype(jnp.bfloat16), tile) + NOISE_LEVEL * current
        moments = jnp.stack(
            [
                jnp.sum(current * kernel_image, axis=1),
                jnp.sum(kernel_image * kernel_image, axis=1),
                jnp.sum(previous * kernel_image, axis=1),
                jnp.sum(current * previous, axis=1),
                jnp.sum(current * current, axis=1),
                jnp.sum(previous * previous, axis=1),
            ]
        )
        moments = lax.psum(moments, ("grp", "row"))
        alpha_now = moments[0]
        residual_sq = (
            moments[1]
            + alpha_now * alpha_now * moments[4]
            + beta_prev * beta_prev * moments[5]
            - 2.0 * alpha_now * moments[0]
            - 2.0 * beta_prev * moments[2]
            + 2.0 * alpha_now * beta_prev * moments[3]
        )
        residual = kernel_image - alpha_now[:, None] * current - beta_prev[:, None] * previous
        basis_list.append(current)
        alpha_list.append(alpha_now)
        if iteration + 1 < ITERS:
            beta_now = jnp.sqrt(jnp.maximum(residual_sq, 0.0) + FLOOR_BETA)
            beta_list.append(beta_now)
            previous = current
            current = residual / beta_now[:, None]
            beta_prev = beta_now
    logdet, scale_grad, coefficients = quadrature(jnp.stack(alpha_list), jnp.stack(beta_list))
    solves = scale_root * jnp.einsum("jp,jpn->pn", coefficients, jnp.stack(basis_list))
    return (solves, logdet, scale_grad)


def power_of_two(value):
    return value & (value - 1) == 0


def solution(mesh):
    groups, lines = mesh.shape["grp"], mesh.shape["row"]

    def local(embeds, w_hidden, b_hidden, w_out, probes):
        rows = embeds.shape[0] * groups * lines
        fits = (
            rows * rows <= KERNEL_BYTES
            and lines % 2 == 0
            and power_of_two(groups)
            and power_of_two(lines)
            and probes.shape[1] == LANES
            and w_out.shape[1] == LANES
            and probes.shape[0] % 16 == 0
        )
        step = replicated if fits else distributed
        return step(embeds, w_hidden, b_hidden, w_out, probes)

    return jax.shard_map(
        local,
        mesh=mesh,
        in_specs=(P(("grp", "row"), None), P(), P(), P(), P(None, ("grp", "row"))),
        out_specs=(P(None, ("grp", "row")), P(), P()),
        check_vma=False,
    )
```

```python
import functools
import math

import jax
import jax.numpy as jnp
from jax import lax
from jax.experimental import pallas as pl
from jax.experimental.pallas import tpu as pltpu
from jax.sharding import PartitionSpec as P

ITERS = 8
SWEEPS = 6
INV_WIDTH = 1.0 / 12.0
NOISE_LEVEL = 0.5
FLOOR_BETA = 0.01
EIGEN_FLOOR = 0.25
LANES = 128
TINY = 1e-30
KERNEL_BYTES = 40 * 2**20


def head_kernel(*refs):
    sources, (out_ref, *places, sems) = refs[:5], refs[5:]
    copies = [
        pltpu.make_async_copy(source, place, sems.at[k])
        for k, (source, place) in enumerate(zip(sources, places))
    ]
    for copy in copies:
        copy.start()
    embeds, w_hidden, b_hidden, w_out, probes = places
    rows = embeds.shape[0]
    for copy in copies:
        copy.wait()
    hidden = jax.nn.gelu(
        jnp.dot(embeds[...], w_hidden[...], preferred_element_type=jnp.float32)
        + b_hidden[...][None, :]
    ).astype(jnp.bfloat16)
    out_ref[:rows, :] = jnp.dot(
        hidden, w_out[...], preferred_element_type=jnp.float32
    ).astype(jnp.bfloat16)
    out_ref[rows:, :] = probes[...].astype(jnp.float32).astype(jnp.bfloat16)


def head(*arrays):
    embeds, w_out, probes = arrays[0], arrays[3], arrays[4]
    shape = (embeds.shape[0] + probes.shape[0], w_out.shape[1])
    return pl.pallas_call(
        head_kernel,
        out_shape=pltpu.VMEM(shape, jnp.bfloat16),
        in_specs=[pl.BlockSpec(memory_space=pl.ANY)] * len(arrays),
        out_specs=pl.BlockSpec(memory_space=pltpu.VMEM),
        scratch_shapes=[pltpu.VMEM(a.shape, a.dtype) for a in arrays]
        + [pltpu.SemaphoreType.DMA((len(arrays),))],
    )(*arrays)


def swap(value, axis, flip):
    size = lax.axis_size(axis)
    return lax.ppermute(value, axis, [(i, i ^ flip) for i in range(size)])


def gather_half(block):
    def spread(value, axis, stride):
        far = range(1, lax.axis_size(axis) // stride)
        return jnp.concatenate([value] + [swap(value, axis, stride * k) for k in far])

    return spread(spread(block[None], "row", 2), "grp", 1)


def partner(value):
    return swap(value, "row", 1)


def pairs_of_round(order, turn):
    ring = order - 1
    pairs = [(ring, turn)]
    for gap in range(1, order // 2):
        pairs.append(((turn + gap) % ring, (turn - gap) % ring))
    return [tuple(sorted(pair)) for pair in pairs]


def jacobi_round(entries, columns, pairs):
    entries, columns = dict(entries), list(columns)

    def key(i, j):
        return (i, j) if i <= j else (j, i)

    turns = []
    for p, q in pairs:
        double = 2.0 * entries[p, q]
        gap = entries[q, q] - entries[p, p]
        square = gap * gap + double * double
        live = square > TINY
        inverse = lax.rsqrt(jnp.where(live, square, 1.0))
        width = jnp.where(live, square * inverse, 0.0)
        cos_square = jnp.where(live, 0.5 + 0.5 * jnp.abs(gap) * inverse, 1.0)
        sine_half = jnp.where(live, 0.5 * double * inverse, 0.0)
        upward = gap >= 0.0
        secant = lax.rsqrt(cos_square)
        cosine = cos_square * secant
        sine = jnp.where(upward, sine_half, -sine_half) * secant
        turns.append((cosine, sine, jnp.where(upward, width, -width)))
    for (p, q), (cosine, sine, width) in zip(pairs, turns):
        middle = entries[p, p] + entries[q, q]
        entries[p, p] = 0.5 * (middle - width)
        entries[q, q] = 0.5 * (middle + width)
        entries[p, q] = jnp.zeros_like(width)
        col_p, col_q = columns[p], columns[q]
        columns[p] = cosine * col_p - sine * col_q
        columns[q] = sine * col_p + cosine * col_q
    for a in range(len(pairs)):
        for b in range(a + 1, len(pairs)):
            (p, q), (r, s) = pairs[a], pairs[b]
            cos_a, sin_a, _ = turns[a]
            cos_b, sin_b, _ = turns[b]
            pr, ps = entries[key(p, r)], entries[key(p, s)]
            qr, qs = entries[key(q, r)], entries[key(q, s)]
            pr, qr = cos_a * pr - sin_a * qr, sin_a * pr + cos_a * qr
            ps, qs = cos_a * ps - sin_a * qs, sin_a * ps + cos_a * qs
            pr, ps = cos_b * pr - sin_b * ps, sin_b * pr + cos_b * ps
            qr, qs = cos_b * qr - sin_b * qs, sin_b * qr + cos_b * qs
            entries[key(p, r)], entries[key(p, s)] = pr, ps
            entries[key(q, r)], entries[key(q, s)] = qr, qs
    return entries, columns


def quadrature_lanes(alphas, betas, order):
    shape = alphas[0].shape
    keys = [(i, j) for i in range(order) for j in range(i, order)]
    entries = {}
    for i, j in keys:
        if i == j:
            entries[i, j] = alphas[i]
        elif j == i + 1:
            entries[i, j] = betas[i]
        else:
            entries[i, j] = jnp.zeros(shape, jnp.float32)
    sublane = lax.broadcasted_iota(jnp.int32, shape, 0)
    columns = [jnp.where(sublane == k, 1.0, 0.0).astype(jnp.float32) for k in range(order)]

    def sweep(_, state):
        values, columns = state
        entries = dict(zip(keys, values))
        for turn in range(order - 1):
            entries, columns = jacobi_round(entries, columns, pairs_of_round(order, turn))
        return tuple(entries[k] for k in keys), tuple(columns)

    values, columns = lax.fori_loop(
        0, SWEEPS, sweep, (tuple(entries[k] for k in keys), tuple(columns))
    )
    entries = dict(zip(keys, values))
    logdet = jnp.zeros((1, shape[1]), jnp.float32)
    coef = jnp.zeros(shape, jnp.float32)
    for k in range(order):
        eigen = jnp.maximum(entries[k, k][:1], EIGEN_FLOOR)
        leading = columns[k][:1]
        logdet = logdet + leading * leading * jnp.log(eigen)
        coef = coef + columns[k] * (leading / eigen)
    return logdet, coef


def split3(value):
    high = value.astype(jnp.bfloat16)
    rest = value - high.astype(jnp.float32)
    mid = rest.astype(jnp.bfloat16)
    low = (rest - mid.astype(jnp.float32)).astype(jnp.bfloat16)
    return high, mid, low


def slot_of(index):
    lines = lax.axis_size("row") // 2
    line, group = lax.axis_index("row") // 2, lax.axis_index("grp")
    return (group ^ (index // lines)) * lines + (line ^ (index % lines))


def place_kernel(blocks, left, right, start_vec):
    count, block_rows, feat = blocks.shape
    probes = start_vec.shape[0]
    local = block_rows - probes
    rows, deep = right.shape
    root = math.sqrt(2 * rows)
    lane = lax.broadcasted_iota(jnp.int32, (local, LANES), 1)
    adder = jnp.ones((2 * feat, LANES), jnp.bfloat16)

    def extra(parts, first, ones):
        total = jnp.where((lane >= ones) & (lane < ones + 3), 1.0, 0.0)
        for k, part in enumerate(parts):
            total = jnp.where(lane == first + k, part.astype(jnp.float32), total)
        return total.astype(jnp.bfloat16)

    def place(index, carry):
        start = pl.multiple_of(slot_of(index) * local, local)
        feats = blocks[index, :local, :]
        wide = feats.astype(jnp.float32)
        square = wide * wide
        high = square.astype(jnp.bfloat16)
        low = (square - high.astype(jnp.float32)).astype(jnp.bfloat16)
        total = jnp.dot(
            jnp.concatenate([high, low], axis=1), adder, preferred_element_type=jnp.float32
        )
        norms = split3(-0.5 * total)
        left[pl.ds(start, local), :feat] = feats
        left[pl.ds(start, local), feat:] = extra(norms, 0, 3)
        right[pl.ds(start, local), :feat] = feats
        right[pl.ds(start, local), feat:] = extra(norms, 3, 0)
        bits = blocks[index, local:, :].astype(jnp.float32)
        start_vec[:, pl.ds(start, local)] = (2.0 * bits - 1.0) / root
        return carry

    lax.fori_loop(0, count, place, 0, unroll=8)
    for k in range(rows // deep):
        left[rows + k * probes : rows + (k + 1) * probes, :] = start_vec[
            :, k * deep : (k + 1) * deep
        ].astype(jnp.bfloat16)


def form(left, right, kern, symmetric=False):
    size = 512
    rows = right.shape[0]
    for start in range(0, rows, size):
        block = right[start : start + size, :]
        for top in range(start if symmetric else 0, rows, size):
            inner = lax.dot_general(
                left[top : top + size, :],
                block,
                (((1,), (1,)), ((), ())),
                preferred_element_type=jnp.float32,
            )
            tile = jnp.exp2(
                jnp.minimum(inner, 0.0) * (2.0 * INV_WIDTH * math.log2(math.e))
            ).astype(jnp.bfloat16)
            kern[top : top + size, start : start + size] = tile
            if symmetric and top > start:
                kern[start : start + size, top : top + size] = tile.T


def product(vectors, kern):
    count = vectors[0].shape[0]
    pieces = jnp.concatenate([piece for vector in vectors for piece in split3(vector)])
    width = 512
    parts = [[] for _ in vectors]
    for start in range(0, kern.shape[1], width):
        whole = jnp.dot(
            pieces, kern[:, start : start + width], preferred_element_type=jnp.float32
        )
        for k, part in enumerate(parts):
            high, mid, low = (
                whole[(3 * k + i) * count : (3 * k + i + 1) * count] for i in range(3)
            )
            part.append(high + (mid + low))
    return [jnp.concatenate(part, axis=1) for part in parts]


def first_product(low, kern, image, base=None):
    width = 512
    for start in range(0, image.shape[1], width):
        here = slice(start, start + width)
        part = jnp.dot(low, kern[:, here], preferred_element_type=jnp.float32)
        image[:, here] = part if base is None else base[:, here] + part


def form_own_kernel(left, right, own, kern, image):
    form(left, right, kern, symmetric=True)
    first_product(own[...].astype(jnp.bfloat16), kern, image)


def form_oth_kernel(left, right, image_own, kern, oth, image):
    form(left, right, kern)
    probes, (rows, deep) = oth.shape[0], right.shape
    low = jnp.concatenate(
        [left[rows + k * probes : rows + (k + 1) * probes, :] for k in range(rows // deep)], axis=1
    )
    oth[...] = low.astype(jnp.float32)
    first_product(low, kern, image, image_own)


def row_sum(first, second):
    return jnp.sum(first * second, axis=1, keepdims=True)


def ahead_kernel(*refs, step):
    if step > 1:
        before_own, table, *refs = refs
    own, image_own, kern_own, ahead, along = refs
    q_own = own[...]
    u_own = image_own[...] + NOISE_LEVEL * q_own
    if step > 1:
        u_own = u_own - table[:, ITERS + step - 2 : ITERS + step - 1] * before_own[...]
    ahead[...], along[...] = product([u_own, q_own], kern_own)


def step_kernel(*refs, step):
    if step > 1:
        before_own, before_oth, table, *refs = refs
    own, oth, image_own, image_oth, ahead, along, kern_oth, *outs = refs
    next_own, next_oth, image, table_out = outs
    lane = lax.broadcasted_iota(jnp.int32, table_out.shape, 1)
    q_own, q_oth = own[...], oth[...]
    w_own = image_own[...] + NOISE_LEVEL * q_own
    w_oth = image_oth[...] + NOISE_LEVEL * q_oth
    u_own, u_oth, last = w_own, w_oth, jnp.zeros(table_out.shape, jnp.float32)
    if step > 1:
        last = table[...]
        beta = last[:, ITERS + step - 2 : ITERS + step - 1]
        u_own = u_own - beta * before_own[...]
        u_oth = u_oth - beta * before_oth[...]
    ahead_oth, along_oth = product([u_oth, q_oth], kern_oth)
    alpha = row_sum(q_own, w_own) + row_sum(q_oth, w_oth)
    r_own, r_oth = u_own - alpha * q_own, u_oth - alpha * q_oth
    beta = jnp.sqrt(
        jnp.maximum(row_sum(r_own, r_own) + row_sum(r_oth, r_oth), 0.0) + FLOOR_BETA
    )
    next_own[...], next_oth[...] = r_own / beta, r_oth / beta
    table_out[...] = jnp.where(
        lane == step - 1, alpha, jnp.where(lane == ITERS + step - 1, beta, last)
    )
    image[...] = (ahead[...] + ahead_oth - alpha * (along[...] + along_oth)) / beta


def finish_kernel(*refs):
    table, oth, image_own, image_oth, *basis = refs[: 4 + ITERS]
    solves, logdet_ref, scale_ref, square = refs[4 + ITERS :]
    probes, local = solves.shape
    root = math.sqrt(2 * oth.shape[1])
    own = basis[-1]
    alpha = row_sum(own[...], image_own[...] + NOISE_LEVEL * own[...]) + row_sum(
        oth[...], image_oth[...] + NOISE_LEVEL * oth[...]
    )
    lane = lax.broadcasted_iota(jnp.int32, table.shape, 1)
    square[...] = jnp.zeros_like(square)
    square[:probes, :] = jnp.where(lane == ITERS - 1, alpha, table[...])
    turned = jnp.transpose(square[...])
    spread = lambda j: jnp.broadcast_to(turned[j : j + 1, :], (8, LANES))
    logdet, coef = quadrature_lanes(
        [spread(j) for j in range(ITERS)], [spread(ITERS + j) for j in range(ITERS - 1)], ITERS
    )
    logdet_ref[...] = logdet[0, :probes]
    scale_ref[...] = 1.0 - NOISE_LEVEL * coef[0, :probes]
    square[:ITERS, :] = coef
    weights = jnp.transpose(square[...])[:probes, :]
    mine = pl.multiple_of(slot_of(0) * local, local)
    total = jnp.zeros((probes, local), jnp.float32)
    for j in range(ITERS):
        total = total + weights[:, j : j + 1] * basis[j][:, pl.ds(mine, local)]
    solves[...] = root * total


def call(kernel, outs, scratch=()):
    return pl.pallas_call(
        kernel,
        out_shape=[jax.ShapeDtypeStruct(shape, dtype) for shape, dtype in outs],
        scratch_shapes=[pltpu.VMEM(shape, dtype) for shape, dtype in scratch],
        compiler_params=pltpu.CompilerParams(vmem_limit_bytes=16 * 2**20),
    )


def replicated(embeds, w_hidden, b_hidden, w_out, probes):
    count, local = probes.shape
    low, wide = jnp.bfloat16, jnp.float32
    block_own = gather_half(head(embeds, w_hidden, b_hidden, w_out, probes))
    half = block_own.shape[0] * local
    deep = w_out.shape[1] + LANES
    vector, square, table = ((count, half), wide), ((half, half), low), ((count, LANES), wide)
    carrier = ((half + count * half // deep, deep), low)
    left, right, own = call(place_kernel, [carrier, ((half, deep), low), vector])(block_own)
    left_oth = partner(left)
    kern_own, image = call(form_own_kernel, [square, vector])(left, right, own)
    kern_oth, oth, image = call(form_oth_kernel, [square, vector, vector])(left_oth, right, image)
    basis, before = [own], ()
    for step in range(1, ITERS):
        image_oth = partner(image)
        ahead, along = call(functools.partial(ahead_kernel, step=step), [vector, vector])(
            *before[::2], own, image, kern_own
        )
        after_own, after_oth, image, rates = call(
            functools.partial(step_kernel, step=step), [vector, vector, vector, table]
        )(*before, own, oth, image, image_oth, ahead, along, kern_oth)
        before = (own, oth, rates)
        own, oth = after_own, after_oth
        basis.append(own)
    return call(
        finish_kernel,
        [((count, local), wide), ((count,), wide), ((count,), wide)],
        [((LANES, LANES), wide)],
    )(rates, oth, image, partner(image), *basis)


def rotate(matrix, vectors, first_idx, second_idx):
    diag_first = matrix[first_idx, first_idx]
    diag_second = matrix[second_idx, second_idx]
    off_value = matrix[first_idx, second_idx]
    half_angle = 0.5 * jnp.arctan2(2.0 * off_value, diag_first - diag_second)
    cosine = jnp.cos(half_angle)
    sine_val = jnp.sin(half_angle)
    row_first = matrix[first_idx]
    row_second = matrix[second_idx]
    matrix = matrix.at[first_idx].set(cosine * row_first + sine_val * row_second)
    matrix = matrix.at[second_idx].set(cosine * row_second - sine_val * row_first)
    col_first = matrix[:, first_idx]
    col_second = matrix[:, second_idx]
    matrix = matrix.at[:, first_idx].set(cosine * col_first + sine_val * col_second)
    matrix = matrix.at[:, second_idx].set(cosine * col_second - sine_val * col_first)
    vec_first = vectors[:, first_idx]
    vec_second = vectors[:, second_idx]
    vectors = vectors.at[:, first_idx].set(cosine * vec_first + sine_val * vec_second)
    vectors = vectors.at[:, second_idx].set(cosine * vec_second - sine_val * vec_first)
    return (matrix, vectors)


def quadrature(alphas, betas):
    tri_order = alphas.shape[0]
    identity = jnp.eye(tri_order, dtype=jnp.float32)
    upper_band = jnp.concatenate([jnp.zeros_like(alphas[:1]), betas], axis=0)
    shifted = jnp.eye(tri_order, k=1, dtype=jnp.float32)[:, :, None] * upper_band[None, :, :]
    matrix = identity[:, :, None] * alphas[None, :, :] + shifted + jnp.transpose(shifted, (1, 0, 2))
    vectors = jnp.broadcast_to(identity[:, :, None], matrix.shape)
    for sweep_index in range(SWEEPS):
        for first_idx in range(tri_order):
            for second_idx in range(first_idx + 1, tri_order):
                matrix, vectors = rotate(matrix, vectors, first_idx, second_idx)
    eigenvalues = jnp.maximum(jnp.sum(matrix * identity[:, :, None], axis=1), EIGEN_FLOOR)
    leading = vectors[0]
    logdet = jnp.sum(jnp.square(leading) * jnp.log(eigenvalues), axis=0)
    coefficients = jnp.sum(vectors * (leading / eigenvalues)[None, :, :], axis=1)
    scale_grad = 1.0 - NOISE_LEVEL * coefficients[0]
    return (logdet, scale_grad, coefficients)


def kernel_block(row_feats, row_norms, col_block, norm_block):
    inner = lax.dot_general(
        row_feats, col_block, (((1,), (1,)), ((), ())), preferred_element_type=jnp.float32
    )
    distance = row_norms[:, None] + norm_block[None, :] - 2.0 * inner
    return jnp.exp(-jnp.maximum(distance, 0.0) * INV_WIDTH).astype(jnp.bfloat16)


def block_width():
    return 512


def form_tile(row_feats, row_norms, col_feats, col_norms):
    total_cols = col_feats.shape[0]
    step_cols = block_width()
    block_count = total_cols // step_cols

    def one_block(block_index, tile):
        offset = block_index * step_cols
        col_block = lax.dynamic_slice_in_dim(col_feats, offset, step_cols, 0)
        norm_block = lax.dynamic_slice_in_dim(col_norms, offset, step_cols, 0)
        block = kernel_block(row_feats, row_norms, col_block, norm_block)
        return lax.dynamic_update_slice_in_dim(tile, block, offset, 1)

    empty = jnp.zeros((row_feats.shape[0], total_cols), jnp.bfloat16)
    return lax.fori_loop(0, block_count, one_block, empty)


def apply_kernel(vectors_low, tile):
    partial_value = lax.dot_general(
        lax.all_gather(vectors_low, "row", axis=1, tiled=True),
        tile,
        (((1,), (1,)), ((), ())),
        preferred_element_type=jnp.float32,
    )
    return lax.psum_scatter(partial_value, "grp", scatter_dimension=1, tiled=True)


def distributed(embeds, w_hidden, b_hidden, w_out, probes):
    hidden = jax.nn.gelu(
        jnp.dot(embeds, w_hidden, preferred_element_type=jnp.float32) + b_hidden
    ).astype(jnp.bfloat16)
    features = jnp.dot(hidden, w_out, preferred_element_type=jnp.float32).astype(jnp.bfloat16)
    row_feats = lax.all_gather(features, "grp", axis=0, tiled=True)
    col_feats = lax.all_gather(features, "row", axis=0, tiled=True)
    row_norms = jnp.sum(jnp.square(row_feats.astype(jnp.float32)), axis=1)
    col_norms = jnp.sum(jnp.square(col_feats.astype(jnp.float32)), axis=1)
    tile = form_tile(row_feats, row_norms, col_feats, col_norms)
    total_rows = probes.shape[1] * lax.axis_size("grp") * lax.axis_size("row")
    scale_root = math.sqrt(total_rows)
    current = (2 * probes - 1).astype(jnp.float32) / scale_root
    previous = jnp.zeros_like(current)
    beta_prev = jnp.zeros((current.shape[0],), jnp.float32)
    basis_list = []
    alpha_list = []
    beta_list = []
    for iteration in range(ITERS):
        kernel_image = apply_kernel(current.astype(jnp.bfloat16), tile) + NOISE_LEVEL * current
        moments = jnp.stack(
            [
                jnp.sum(current * kernel_image, axis=1),
                jnp.sum(kernel_image * kernel_image, axis=1),
                jnp.sum(previous * kernel_image, axis=1),
                jnp.sum(current * previous, axis=1),
                jnp.sum(current * current, axis=1),
                jnp.sum(previous * previous, axis=1),
            ]
        )
        moments = lax.psum(moments, ("grp", "row"))
        alpha_now = moments[0]
        residual_sq = (
            moments[1]
            + alpha_now * alpha_now * moments[4]
            + beta_prev * beta_prev * moments[5]
            - 2.0 * alpha_now * moments[0]
            - 2.0 * beta_prev * moments[2]
            + 2.0 * alpha_now * beta_prev * moments[3]
        )
        residual = kernel_image - alpha_now[:, None] * current - beta_prev[:, None] * previous
        basis_list.append(current)
        alpha_list.append(alpha_now)
        if iteration + 1 < ITERS:
            beta_now = jnp.sqrt(jnp.maximum(residual_sq, 0.0) + FLOOR_BETA)
            beta_list.append(beta_now)
            previous = current
            current = residual / beta_now[:, None]
            beta_prev = beta_now
    logdet, scale_grad, coefficients = quadrature(jnp.stack(alpha_list), jnp.stack(beta_list))
    solves = scale_root * jnp.einsum("jp,jpn->pn", coefficients, jnp.stack(basis_list))
    return (solves, logdet, scale_grad)


def power_of_two(value):
    return value & (value - 1) == 0


def solution(mesh):
    groups, lines = mesh.shape["grp"], mesh.shape["row"]

    def local(embeds, w_hidden, b_hidden, w_out, probes):
        rows = embeds.shape[0] * groups * lines
        fits = (
            rows * rows <= KERNEL_BYTES
            and lines % 2 == 0
            and power_of_two(groups)
            and power_of_two(lines)
            and probes.shape[1] == LANES
            and w_out.shape[1] == LANES
            and probes.shape[0] % 16 == 0
        )
        step = replicated if fits else distributed
        return step(embeds, w_hidden, b_hidden, w_out, probes)

    return jax.shard_map(
        local,
        mesh=mesh,
        in_specs=(P(("grp", "row"), None), P(), P(), P(), P(None, ("grp", "row"))),
        out_specs=(P(None, ("grp", "row")), P(), P()),
        check_vma=False,
    )
```

```python
import functools
import math

import jax
import jax.numpy as jnp
from jax import lax
from jax.experimental import pallas as pl
from jax.experimental.pallas import tpu as pltpu
from jax.sharding import PartitionSpec as P

ITERS = 8
SWEEPS = 6
INV_WIDTH = 1.0 / 12.0
NOISE_LEVEL = 0.5
FLOOR_BETA = 0.01
EIGEN_FLOOR = 0.25
LANES = 128
TINY = 1e-15
KERNEL_BYTES = 40 * 2**20


def head_kernel(*refs):
    sources, (out_ref, *places, sems) = refs[:5], refs[5:]
    copies = [
        pltpu.make_async_copy(source, place, sems.at[k])
        for k, (source, place) in enumerate(zip(sources, places))
    ]
    for copy in copies:
        copy.start()
    embeds, w_hidden, b_hidden, w_out, probes = places
    rows = embeds.shape[0]
    for copy in copies:
        copy.wait()
    hidden = jax.nn.gelu(
        jnp.dot(embeds[...], w_hidden[...], preferred_element_type=jnp.float32)
        + b_hidden[...][None, :]
    ).astype(jnp.bfloat16)
    out_ref[:rows, :] = jnp.dot(
        hidden, w_out[...], preferred_element_type=jnp.float32
    ).astype(jnp.bfloat16)
    out_ref[rows:, :] = probes[...].astype(jnp.float32).astype(jnp.bfloat16)


def head(*arrays):
    embeds, w_out, probes = arrays[0], arrays[3], arrays[4]
    shape = (embeds.shape[0] + probes.shape[0], w_out.shape[1])
    return pl.pallas_call(
        head_kernel,
        out_shape=pltpu.VMEM(shape, jnp.bfloat16),
        in_specs=[pl.BlockSpec(memory_space=pl.ANY)] * len(arrays),
        out_specs=pl.BlockSpec(memory_space=pltpu.VMEM),
        scratch_shapes=[pltpu.VMEM(a.shape, a.dtype) for a in arrays]
        + [pltpu.SemaphoreType.DMA((len(arrays),))],
    )(*arrays)


def swap(value, axis, flip):
    size = lax.axis_size(axis)
    return lax.ppermute(value, axis, [(i, i ^ flip) for i in range(size)])


def gather_half(block):
    def spread(value, axis, stride):
        far = range(1, lax.axis_size(axis) // stride)
        return jnp.concatenate([value] + [swap(value, axis, stride * k) for k in far])

    return spread(spread(block[None], "row", 2), "grp", 1)


def partner(value):
    return swap(value, "row", 1)


def pairs_of_round(order, turn):
    ring = order - 1
    pairs = [(ring, turn)]
    for gap in range(1, order // 2):
        pairs.append(((turn + gap) % ring, (turn - gap) % ring))
    return [tuple(sorted(pair)) for pair in pairs]


def jacobi_round(entries, columns, pairs):
    entries, columns = dict(entries), list(columns)

    def key(i, j):
        return (i, j) if i <= j else (j, i)

    turns = []
    for p, q in pairs:
        off = entries[p, q]
        gap = entries[q, q] - entries[p, p]
        size = jnp.abs(gap) + TINY
        square = size * size + 4.0 * (off * off)
        inverse = lax.rsqrt(square)
        cos_square = 0.5 + 0.5 * size * inverse
        secant = lax.rsqrt(cos_square)
        signed = jnp.where(gap >= 0.0, inverse, -inverse)
        turns.append((cos_square * secant, off * signed * secant, square * signed))
    for (p, q), (cosine, sine, width) in zip(pairs, turns):
        middle = entries[p, p] + entries[q, q]
        entries[p, p] = 0.5 * (middle - width)
        entries[q, q] = 0.5 * (middle + width)
        entries[p, q] = jnp.zeros_like(width)
        col_p, col_q = columns[p], columns[q]
        columns[p] = cosine * col_p - sine * col_q
        columns[q] = sine * col_p + cosine * col_q
    for a in range(len(pairs)):
        for b in range(a + 1, len(pairs)):
            (p, q), (r, s) = pairs[a], pairs[b]
            cos_a, sin_a, _ = turns[a]
            cos_b, sin_b, _ = turns[b]
            pr, ps = entries[key(p, r)], entries[key(p, s)]
            qr, qs = entries[key(q, r)], entries[key(q, s)]
            pr, qr = cos_a * pr - sin_a * qr, sin_a * pr + cos_a * qr
            ps, qs = cos_a * ps - sin_a * qs, sin_a * ps + cos_a * qs
            pr, ps = cos_b * pr - sin_b * ps, sin_b * pr + cos_b * ps
            qr, qs = cos_b * qr - sin_b * qs, sin_b * qr + cos_b * qs
            entries[key(p, r)], entries[key(p, s)] = pr, ps
            entries[key(q, r)], entries[key(q, s)] = qr, qs
    return entries, columns


def quadrature_lanes(alphas, betas, order):
    shape = alphas[0].shape
    keys = [(i, j) for i in range(order) for j in range(i, order)]
    entries = {}
    for i, j in keys:
        if i == j:
            entries[i, j] = alphas[i]
        elif j == i + 1:
            entries[i, j] = betas[i]
        else:
            entries[i, j] = jnp.zeros(shape, jnp.float32)
    sublane = lax.broadcasted_iota(jnp.int32, shape, 0)
    columns = [jnp.where(sublane == k, 1.0, 0.0).astype(jnp.float32) for k in range(order)]

    def sweep(_, state):
        values, columns = state
        entries = dict(zip(keys, values))
        for turn in range(order - 1):
            entries, columns = jacobi_round(entries, columns, pairs_of_round(order, turn))
        return tuple(entries[k] for k in keys), tuple(columns)

    values, columns = lax.fori_loop(
        0, SWEEPS, sweep, (tuple(entries[k] for k in keys), tuple(columns))
    )
    entries = dict(zip(keys, values))
    logdet = jnp.zeros((1, shape[1]), jnp.float32)
    coef = jnp.zeros(shape, jnp.float32)
    for k in range(order):
        eigen = jnp.maximum(entries[k, k][:1], EIGEN_FLOOR)
        leading = columns[k][:1]
        logdet = logdet + leading * leading * jnp.log(eigen)
        coef = coef + columns[k] * (leading / eigen)
    return logdet, coef


def split3(value):
    high = value.astype(jnp.bfloat16)
    rest = value - high.astype(jnp.float32)
    mid = rest.astype(jnp.bfloat16)
    low = (rest - mid.astype(jnp.float32)).astype(jnp.bfloat16)
    return high, mid, low


def slot_of(index):
    lines = lax.axis_size("row") // 2
    line, group = lax.axis_index("row") // 2, lax.axis_index("grp")
    return (group ^ (index // lines)) * lines + (line ^ (index % lines))


def place_kernel(blocks, left, right, start_vec):
    count, block_rows, feat = blocks.shape
    probes = start_vec.shape[0]
    local = block_rows - probes
    rows, deep = right.shape
    root = math.sqrt(2 * rows)
    lane = lax.broadcasted_iota(jnp.int32, (local, LANES), 1)
    adder = jnp.full((2 * feat, LANES), -0.5, jnp.bfloat16)
    ones = jnp.where((lane < 3) | ((lane >= 6) & (lane < 9)), 1.0, 0.0)

    def rounded(value):
        return value.astype(jnp.bfloat16).astype(jnp.float32)

    def place(index, carry):
        start = pl.multiple_of(slot_of(index) * local, local)
        here = pl.ds(start, local)
        feats = blocks[index, :local, :]
        wide = feats.astype(jnp.float32)
        square = wide * wide
        high = square.astype(jnp.bfloat16)
        low = (square - high.astype(jnp.float32)).astype(jnp.bfloat16)
        total = jnp.dot(
            jnp.concatenate([high, low], axis=1), adder, preferred_element_type=jnp.float32
        )
        rest = total - rounded(total)
        pieces = jnp.where(lane == 3, total, jnp.where(lane == 4, rest, rest - rounded(rest)))
        pieces = jnp.where((lane >= 3) & (lane < 6), pieces, ones)
        left[here, :feat] = feats
        left[here, feat:] = pieces.astype(jnp.bfloat16)
        right[here, :feat] = feats
        right[here, feat:] = pltpu.roll(pieces, LANES - 3, 1).astype(jnp.bfloat16)
        bits = blocks[index, local:, :].astype(jnp.float32)
        start_vec[:, here] = (2.0 * bits - 1.0) / root
        return carry

    lax.fori_loop(0, count, place, 0, unroll=16)
    for k in range(rows // deep):
        left[rows + k * probes : rows + (k + 1) * probes, :] = start_vec[
            :, k * deep : (k + 1) * deep
        ].astype(jnp.bfloat16)


def form(left, right, kern, symmetric=False):
    size = 512
    rows = right.shape[0]
    for start in range(0, rows, size):
        block = right[start : start + size, :]
        for top in range(start if symmetric else 0, rows, size):
            inner = lax.dot_general(
                left[top : top + size, :],
                block,
                (((1,), (1,)), ((), ())),
                preferred_element_type=jnp.float32,
            )
            tile = jnp.exp2(
                jnp.minimum(inner, 0.0) * (2.0 * INV_WIDTH * math.log2(math.e))
            ).astype(jnp.bfloat16)
            kern[top : top + size, start : start + size] = tile
            if symmetric and top > start:
                kern[start : start + size, top : top + size] = tile.T


def product(vectors, kern):
    count = vectors[0].shape[0]
    pieces = jnp.concatenate([piece for vector in vectors for piece in split3(vector)])
    width = 512
    parts = [[] for _ in vectors]
    for start in range(0, kern.shape[1], width):
        whole = jnp.dot(
            pieces, kern[:, start : start + width], preferred_element_type=jnp.float32
        )
        for k, part in enumerate(parts):
            high, mid, low = (
                whole[(3 * k + i) * count : (3 * k + i + 1) * count] for i in range(3)
            )
            part.append(high + (mid + low))
    return [jnp.concatenate(part, axis=1) for part in parts]


def first_product(low, kern, image, base=None):
    width = 512
    for start in range(0, image.shape[1], width):
        here = slice(start, start + width)
        part = jnp.dot(low, kern[:, here], preferred_element_type=jnp.float32)
        image[:, here] = part if base is None else base[:, here] + part


def form_own_kernel(left, right, own, kern, image):
    form(left, right, kern, symmetric=True)
    first_product(own[...].astype(jnp.bfloat16), kern, image)


def form_oth_kernel(left, right, image_own, kern, oth, image):
    form(left, right, kern)
    probes, (rows, deep) = oth.shape[0], right.shape
    low = jnp.concatenate(
        [left[rows + k * probes : rows + (k + 1) * probes, :] for k in range(rows // deep)], axis=1
    )
    oth[...] = low.astype(jnp.float32)
    first_product(low, kern, image, image_own)


def row_sum(first, second):
    return jnp.sum(first * second, axis=1, keepdims=True)


def ahead_kernel(*refs, step):
    if step > 1:
        before_own, table, *refs = refs
    own, image_own, kern_own, ahead, along = refs
    q_own = own[...]
    u_own = image_own[...] + NOISE_LEVEL * q_own
    if step > 1:
        u_own = u_own - table[:, ITERS + step - 2 : ITERS + step - 1] * before_own[...]
    ahead[...], along[...] = product([u_own, q_own], kern_own)


def step_kernel(*refs, step):
    if step > 1:
        before_own, before_oth, table, *refs = refs
    own, oth, image_own, image_oth, ahead, along, kern_oth, *outs = refs
    next_own, next_oth, image, table_out = outs
    lane = lax.broadcasted_iota(jnp.int32, table_out.shape, 1)
    q_own, q_oth = own[...], oth[...]
    w_own = image_own[...] + NOISE_LEVEL * q_own
    w_oth = image_oth[...] + NOISE_LEVEL * q_oth
    u_own, u_oth, last = w_own, w_oth, jnp.zeros(table_out.shape, jnp.float32)
    if step > 1:
        last = table[...]
        beta = last[:, ITERS + step - 2 : ITERS + step - 1]
        u_own = u_own - beta * before_own[...]
        u_oth = u_oth - beta * before_oth[...]
    ahead_oth, along_oth = product([u_oth, q_oth], kern_oth)
    alpha = row_sum(q_own, w_own) + row_sum(q_oth, w_oth)
    r_own, r_oth = u_own - alpha * q_own, u_oth - alpha * q_oth
    beta = jnp.sqrt(
        jnp.maximum(row_sum(r_own, r_own) + row_sum(r_oth, r_oth), 0.0) + FLOOR_BETA
    )
    next_own[...], next_oth[...] = r_own / beta, r_oth / beta
    table_out[...] = jnp.where(
        lane == step - 1, alpha, jnp.where(lane == ITERS + step - 1, beta, last)
    )
    image[...] = (ahead[...] + ahead_oth - alpha * (along[...] + along_oth)) / beta


def finish_kernel(*refs):
    table, oth, image_own, image_oth, *basis = refs[: 4 + ITERS]
    solves, logdet_ref, scale_ref, square = refs[4 + ITERS :]
    probes, local = solves.shape
    root = math.sqrt(2 * oth.shape[1])
    own = basis[-1]
    alpha = row_sum(own[...], image_own[...] + NOISE_LEVEL * own[...]) + row_sum(
        oth[...], image_oth[...] + NOISE_LEVEL * oth[...]
    )
    lane = lax.broadcasted_iota(jnp.int32, table.shape, 1)
    square[...] = jnp.zeros_like(square)
    square[:probes, :] = jnp.where(lane == ITERS - 1, alpha, table[...])
    turned = jnp.transpose(square[...])
    spread = lambda j: jnp.broadcast_to(turned[j : j + 1, :], (8, LANES))
    logdet, coef = quadrature_lanes(
        [spread(j) for j in range(ITERS)], [spread(ITERS + j) for j in range(ITERS - 1)], ITERS
    )
    logdet_ref[...] = logdet[0, :probes]
    scale_ref[...] = 1.0 - NOISE_LEVEL * coef[0, :probes]
    square[:ITERS, :] = coef
    weights = jnp.transpose(square[...])[:probes, :]
    mine = pl.multiple_of(slot_of(0) * local, local)
    total = jnp.zeros((probes, local), jnp.float32)
    for j in range(ITERS):
        total = total + weights[:, j : j + 1] * basis[j][:, pl.ds(mine, local)]
    solves[...] = root * total


def call(kernel, outs, scratch=()):
    return pl.pallas_call(
        kernel,
        out_shape=[jax.ShapeDtypeStruct(shape, dtype) for shape, dtype in outs],
        scratch_shapes=[pltpu.VMEM(shape, dtype) for shape, dtype in scratch],
        compiler_params=pltpu.CompilerParams(vmem_limit_bytes=16 * 2**20),
    )


def replicated(embeds, w_hidden, b_hidden, w_out, probes):
    count, local = probes.shape
    low, wide = jnp.bfloat16, jnp.float32
    block_own = gather_half(head(embeds, w_hidden, b_hidden, w_out, probes))
    half = block_own.shape[0] * local
    deep = w_out.shape[1] + LANES
    vector, square, table = ((count, half), wide), ((half, half), low), ((count, LANES), wide)
    carrier = ((half + count * half // deep, deep), low)
    left, right, own = call(place_kernel, [carrier, ((half, deep), low), vector])(block_own)
    left_oth = partner(left)
    kern_own, image = call(form_own_kernel, [square, vector])(left, right, own)
    kern_oth, oth, image = call(form_oth_kernel, [square, vector, vector])(left_oth, right, image)
    basis, before = [own], ()
    for step in range(1, ITERS):
        image_oth = partner(image)
        ahead, along = call(functools.partial(ahead_kernel, step=step), [vector, vector])(
            *before[::2], own, image, kern_own
        )
        after_own, after_oth, image, rates = call(
            functools.partial(step_kernel, step=step), [vector, vector, vector, table]
        )(*before, own, oth, image, image_oth, ahead, along, kern_oth)
        before = (own, oth, rates)
        own, oth = after_own, after_oth
        basis.append(own)
    return call(
        finish_kernel,
        [((count, local), wide), ((count,), wide), ((count,), wide)],
        [((LANES, LANES), wide)],
    )(rates, oth, image, partner(image), *basis)


def rotate(matrix, vectors, first_idx, second_idx):
    diag_first = matrix[first_idx, first_idx]
    diag_second = matrix[second_idx, second_idx]
    off_value = matrix[first_idx, second_idx]
    half_angle = 0.5 * jnp.arctan2(2.0 * off_value, diag_first - diag_second)
    cosine = jnp.cos(half_angle)
    sine_val = jnp.sin(half_angle)
    row_first = matrix[first_idx]
    row_second = matrix[second_idx]
    matrix = matrix.at[first_idx].set(cosine * row_first + sine_val * row_second)
    matrix = matrix.at[second_idx].set(cosine * row_second - sine_val * row_first)
    col_first = matrix[:, first_idx]
    col_second = matrix[:, second_idx]
    matrix = matrix.at[:, first_idx].set(cosine * col_first + sine_val * col_second)
    matrix = matrix.at[:, second_idx].set(cosine * col_second - sine_val * col_first)
    vec_first = vectors[:, first_idx]
    vec_second = vectors[:, second_idx]
    vectors = vectors.at[:, first_idx].set(cosine * vec_first + sine_val * vec_second)
    vectors = vectors.at[:, second_idx].set(cosine * vec_second - sine_val * vec_first)
    return (matrix, vectors)


def quadrature(alphas, betas):
    tri_order = alphas.shape[0]
    identity = jnp.eye(tri_order, dtype=jnp.float32)
    upper_band = jnp.concatenate([jnp.zeros_like(alphas[:1]), betas], axis=0)
    shifted = jnp.eye(tri_order, k=1, dtype=jnp.float32)[:, :, None] * upper_band[None, :, :]
    matrix = identity[:, :, None] * alphas[None, :, :] + shifted + jnp.transpose(shifted, (1, 0, 2))
    vectors = jnp.broadcast_to(identity[:, :, None], matrix.shape)
    for sweep_index in range(SWEEPS):
        for first_idx in range(tri_order):
            for second_idx in range(first_idx + 1, tri_order):
                matrix, vectors = rotate(matrix, vectors, first_idx, second_idx)
    eigenvalues = jnp.maximum(jnp.sum(matrix * identity[:, :, None], axis=1), EIGEN_FLOOR)
    leading = vectors[0]
    logdet = jnp.sum(jnp.square(leading) * jnp.log(eigenvalues), axis=0)
    coefficients = jnp.sum(vectors * (leading / eigenvalues)[None, :, :], axis=1)
    scale_grad = 1.0 - NOISE_LEVEL * coefficients[0]
    return (logdet, scale_grad, coefficients)


def kernel_block(row_feats, row_norms, col_block, norm_block):
    inner = lax.dot_general(
        row_feats, col_block, (((1,), (1,)), ((), ())), preferred_element_type=jnp.float32
    )
    distance = row_norms[:, None] + norm_block[None, :] - 2.0 * inner
    return jnp.exp(-jnp.maximum(distance, 0.0) * INV_WIDTH).astype(jnp.bfloat16)


def block_width():
    return 512


def form_tile(row_feats, row_norms, col_feats, col_norms):
    total_cols = col_feats.shape[0]
    step_cols = block_width()
    block_count = total_cols // step_cols

    def one_block(block_index, tile):
        offset = block_index * step_cols
        col_block = lax.dynamic_slice_in_dim(col_feats, offset, step_cols, 0)
        norm_block = lax.dynamic_slice_in_dim(col_norms, offset, step_cols, 0)
        block = kernel_block(row_feats, row_norms, col_block, norm_block)
        return lax.dynamic_update_slice_in_dim(tile, block, offset, 1)

    empty = jnp.zeros((row_feats.shape[0], total_cols), jnp.bfloat16)
    return lax.fori_loop(0, block_count, one_block, empty)


def apply_kernel(vectors_low, tile):
    partial_value = lax.dot_general(
        lax.all_gather(vectors_low, "row", axis=1, tiled=True),
        tile,
        (((1,), (1,)), ((), ())),
        preferred_element_type=jnp.float32,
    )
    return lax.psum_scatter(partial_value, "grp", scatter_dimension=1, tiled=True)


def distributed(embeds, w_hidden, b_hidden, w_out, probes):
    hidden = jax.nn.gelu(
        jnp.dot(embeds, w_hidden, preferred_element_type=jnp.float32) + b_hidden
    ).astype(jnp.bfloat16)
    features = jnp.dot(hidden, w_out, preferred_element_type=jnp.float32).astype(jnp.bfloat16)
    row_feats = lax.all_gather(features, "grp", axis=0, tiled=True)
    col_feats = lax.all_gather(features, "row", axis=0, tiled=True)
    row_norms = jnp.sum(jnp.square(row_feats.astype(jnp.float32)), axis=1)
    col_norms = jnp.sum(jnp.square(col_feats.astype(jnp.float32)), axis=1)
    tile = form_tile(row_feats, row_norms, col_feats, col_norms)
    total_rows = probes.shape[1] * lax.axis_size("grp") * lax.axis_size("row")
    scale_root = math.sqrt(total_rows)
    current = (2 * probes - 1).astype(jnp.float32) / scale_root
    previous = jnp.zeros_like(current)
    beta_prev = jnp.zeros((current.shape[0],), jnp.float32)
    basis_list = []
    alpha_list = []
    beta_list = []
    for iteration in range(ITERS):
        kernel_image = apply_kernel(current.astype(jnp.bfloat16), tile) + NOISE_LEVEL * current
        moments = jnp.stack(
            [
                jnp.sum(current * kernel_image, axis=1),
                jnp.sum(kernel_image * kernel_image, axis=1),
                jnp.sum(previous * kernel_image, axis=1),
                jnp.sum(current * previous, axis=1),
                jnp.sum(current * current, axis=1),
                jnp.sum(previous * previous, axis=1),
            ]
        )
        moments = lax.psum(moments, ("grp", "row"))
        alpha_now = moments[0]
        residual_sq = (
            moments[1]
            + alpha_now * alpha_now * moments[4]
            + beta_prev * beta_prev * moments[5]
            - 2.0 * alpha_now * moments[0]
            - 2.0 * beta_prev * moments[2]
            + 2.0 * alpha_now * beta_prev * moments[3]
        )
        residual = kernel_image - alpha_now[:, None] * current - beta_prev[:, None] * previous
        basis_list.append(current)
        alpha_list.append(alpha_now)
        if iteration + 1 < ITERS:
            beta_now = jnp.sqrt(jnp.maximum(residual_sq, 0.0) + FLOOR_BETA)
            beta_list.append(beta_now)
            previous = current
            current = residual / beta_now[:, None]
            beta_prev = beta_now
    logdet, scale_grad, coefficients = quadrature(jnp.stack(alpha_list), jnp.stack(beta_list))
    solves = scale_root * jnp.einsum("jp,jpn->pn", coefficients, jnp.stack(basis_list))
    return (solves, logdet, scale_grad)


def power_of_two(value):
    return value & (value - 1) == 0


def solution(mesh):
    groups, lines = mesh.shape["grp"], mesh.shape["row"]

    def local(embeds, w_hidden, b_hidden, w_out, probes):
        rows = embeds.shape[0] * groups * lines
        fits = (
            rows * rows <= KERNEL_BYTES
            and lines % 2 == 0
            and power_of_two(groups)
            and power_of_two(lines)
            and probes.shape[1] == LANES
            and w_out.shape[1] == LANES
            and probes.shape[0] % 16 == 0
        )
        step = replicated if fits else distributed
        return step(embeds, w_hidden, b_hidden, w_out, probes)

    return jax.shard_map(
        local,
        mesh=mesh,
        in_specs=(P(("grp", "row"), None), P(), P(), P(), P(None, ("grp", "row"))),
        out_specs=(P(None, ("grp", "row")), P(), P()),
        check_vma=False,
    )
```

```python
import functools
import math

import jax
import jax.numpy as jnp
from jax import lax
from jax.experimental import pallas as pl
from jax.experimental.pallas import tpu as pltpu
from jax.sharding import PartitionSpec as P

ITERS = 8
SWEEPS = 6
INV_WIDTH = 1.0 / 12.0
NOISE_LEVEL = 0.5
FLOOR_BETA = 0.01
EIGEN_FLOOR = 0.25
LANES = 128
TINY = 1e-15
KERNEL_BYTES = 40 * 2**20


def head_kernel(*refs):
    sources, (out_ref, *places, sems) = refs[:5], refs[5:]
    copies = [
        pltpu.make_async_copy(source, place, sems.at[k])
        for k, (source, place) in enumerate(zip(sources, places))
    ]
    for copy in copies:
        copy.start()
    embeds, w_hidden, b_hidden, w_out, probes = places
    rows = embeds.shape[0]
    for copy in copies:
        copy.wait()
    hidden = jax.nn.gelu(
        jnp.dot(embeds[...], w_hidden[...], preferred_element_type=jnp.float32)
        + b_hidden[...][None, :]
    ).astype(jnp.bfloat16)
    out_ref[:rows, :] = jnp.dot(
        hidden, w_out[...], preferred_element_type=jnp.float32
    ).astype(jnp.bfloat16)
    out_ref[rows:, :] = probes[...].astype(jnp.float32).astype(jnp.bfloat16)


def head(*arrays):
    embeds, w_out, probes = arrays[0], arrays[3], arrays[4]
    shape = (embeds.shape[0] + probes.shape[0], w_out.shape[1])
    return pl.pallas_call(
        head_kernel,
        out_shape=pltpu.VMEM(shape, jnp.bfloat16),
        in_specs=[pl.BlockSpec(memory_space=pl.ANY)] * len(arrays),
        out_specs=pl.BlockSpec(memory_space=pltpu.VMEM),
        scratch_shapes=[pltpu.VMEM(a.shape, a.dtype) for a in arrays]
        + [pltpu.SemaphoreType.DMA((len(arrays),))],
    )(*arrays)


def swap(value, axis, flip):
    size = lax.axis_size(axis)
    return lax.ppermute(value, axis, [(i, i ^ flip) for i in range(size)])


def gather_half(block):
    def spread(value, axis, stride):
        far = range(1, lax.axis_size(axis) // stride)
        return jnp.concatenate([value] + [swap(value, axis, stride * k) for k in far])

    return spread(spread(block[None], "row", 2), "grp", 1)


def partner(value):
    return swap(value, "row", 1)


def pairs_of_round(order, turn):
    ring = order - 1
    pairs = [(ring, turn)]
    for gap in range(1, order // 2):
        pairs.append(((turn + gap) % ring, (turn - gap) % ring))
    return [tuple(sorted(pair)) for pair in pairs]


def jacobi_round(entries, columns, pairs):
    entries, columns = dict(entries), list(columns)

    def key(i, j):
        return (i, j) if i <= j else (j, i)

    turns = []
    for p, q in pairs:
        off = entries[p, q]
        gap = entries[q, q] - entries[p, p]
        size = jnp.abs(gap) + TINY
        square = size * size + 4.0 * (off * off)
        inverse = lax.rsqrt(square)
        cos_square = 0.5 + 0.5 * size * inverse
        secant = lax.rsqrt(cos_square)
        signed = jnp.where(gap >= 0.0, inverse, -inverse)
        turns.append((cos_square * secant, off * signed * secant, square * signed))
    for (p, q), (cosine, sine, width) in zip(pairs, turns):
        middle = entries[p, p] + entries[q, q]
        entries[p, p] = 0.5 * (middle - width)
        entries[q, q] = 0.5 * (middle + width)
        entries[p, q] = jnp.zeros_like(width)
        col_p, col_q = columns[p], columns[q]
        columns[p] = cosine * col_p - sine * col_q
        columns[q] = sine * col_p + cosine * col_q
    for a in range(len(pairs)):
        for b in range(a + 1, len(pairs)):
            (p, q), (r, s) = pairs[a], pairs[b]
            cos_a, sin_a, _ = turns[a]
            cos_b, sin_b, _ = turns[b]
            pr, ps = entries[key(p, r)], entries[key(p, s)]
            qr, qs = entries[key(q, r)], entries[key(q, s)]
            pr, qr = cos_a * pr - sin_a * qr, sin_a * pr + cos_a * qr
            ps, qs = cos_a * ps - sin_a * qs, sin_a * ps + cos_a * qs
            pr, ps = cos_b * pr - sin_b * ps, sin_b * pr + cos_b * ps
            qr, qs = cos_b * qr - sin_b * qs, sin_b * qr + cos_b * qs
            entries[key(p, r)], entries[key(p, s)] = pr, ps
            entries[key(q, r)], entries[key(q, s)] = qr, qs
    return entries, columns


def quadrature_lanes(alphas, betas, order):
    shape = alphas[0].shape
    keys = [(i, j) for i in range(order) for j in range(i, order)]
    entries = {}
    for i, j in keys:
        if i == j:
            entries[i, j] = alphas[i]
        elif j == i + 1:
            entries[i, j] = betas[i]
        else:
            entries[i, j] = jnp.zeros(shape, jnp.float32)
    sublane = lax.broadcasted_iota(jnp.int32, shape, 0)
    columns = [jnp.where(sublane == k, 1.0, 0.0).astype(jnp.float32) for k in range(order)]

    def sweep(_, state):
        values, columns = state
        entries = dict(zip(keys, values))
        for turn in range(order - 1):
            entries, columns = jacobi_round(entries, columns, pairs_of_round(order, turn))
        return tuple(entries[k] for k in keys), tuple(columns)

    values, columns = lax.fori_loop(
        0, SWEEPS, sweep, (tuple(entries[k] for k in keys), tuple(columns))
    )
    entries = dict(zip(keys, values))
    logdet = jnp.zeros((1, shape[1]), jnp.float32)
    coef = jnp.zeros(shape, jnp.float32)
    for k in range(order):
        eigen = jnp.maximum(entries[k, k][:1], EIGEN_FLOOR)
        leading = columns[k][:1]
        logdet = logdet + leading * leading * jnp.log(eigen)
        coef = coef + columns[k] * (leading / eigen)
    return logdet, coef


def split3(value):
    high = value.astype(jnp.bfloat16)
    rest = value - high.astype(jnp.float32)
    mid = rest.astype(jnp.bfloat16)
    low = (rest - mid.astype(jnp.float32)).astype(jnp.bfloat16)
    return high, mid, low


def slot_of(index):
    lines = lax.axis_size("row") // 2
    line, group = lax.axis_index("row") // 2, lax.axis_index("grp")
    return (group ^ (index // lines)) * lines + (line ^ (index % lines))


def place_kernel(blocks, left, right, start_vec):
    count, block_rows, feat = blocks.shape
    probes = start_vec.shape[0]
    local = block_rows - probes
    rows, deep = right.shape
    root = math.sqrt(2 * rows)
    lane = lax.broadcasted_iota(jnp.int32, (local, LANES), 1)
    adder = jnp.full((2 * feat, LANES), -0.5, jnp.bfloat16)
    ones = jnp.where((lane < 3) | ((lane >= 6) & (lane < 9)), 1.0, 0.0)

    def rounded(value):
        return value.astype(jnp.bfloat16).astype(jnp.float32)

    def place(index, carry):
        start = pl.multiple_of(slot_of(index) * local, local)
        here = pl.ds(start, local)
        feats = blocks[index, :local, :]
        wide = feats.astype(jnp.float32)
        square = wide * wide
        high = square.astype(jnp.bfloat16)
        low = (square - high.astype(jnp.float32)).astype(jnp.bfloat16)
        total = jnp.dot(
            jnp.concatenate([high, low], axis=1), adder, preferred_element_type=jnp.float32
        )
        rest = total - rounded(total)
        pieces = jnp.where(lane == 3, total, jnp.where(lane == 4, rest, rest - rounded(rest)))
        pieces = jnp.where((lane >= 3) & (lane < 6), pieces, ones)
        left[here, :feat] = feats
        left[here, feat:] = pieces.astype(jnp.bfloat16)
        right[here, :feat] = feats
        right[here, feat:] = pltpu.roll(pieces, LANES - 3, 1).astype(jnp.bfloat16)
        bits = blocks[index, local:, :].astype(jnp.float32)
        start_vec[:, here] = (2.0 * bits - 1.0) / root
        return carry

    lax.fori_loop(0, count, place, 0, unroll=16)
    for k in range(rows // deep):
        left[rows + k * probes : rows + (k + 1) * probes, :] = start_vec[
            :, k * deep : (k + 1) * deep
        ].astype(jnp.bfloat16)


def form(left, right, kern, symmetric=False):
    size = 256 if symmetric else 1024
    rows = right.shape[0]
    for start in range(0, rows, size):
        block = right[start : start + size, :]
        for top in range(start if symmetric else 0, rows, size):
            inner = lax.dot_general(
                left[top : top + size, :],
                block,
                (((1,), (1,)), ((), ())),
                preferred_element_type=jnp.float32,
            )
            tile = jnp.exp2(
                jnp.minimum(inner, 0.0) * (2.0 * INV_WIDTH * math.log2(math.e))
            ).astype(jnp.bfloat16)
            kern[top : top + size, start : start + size] = tile
            if symmetric and top > start:
                kern[start : start + size, top : top + size] = tile.T


def product(vectors, kern):
    count = vectors[0].shape[0]
    pieces = jnp.concatenate([piece for vector in vectors for piece in split3(vector)])
    width = 512
    parts = [[] for _ in vectors]
    for start in range(0, kern.shape[1], width):
        whole = jnp.dot(
            pieces, kern[:, start : start + width], preferred_element_type=jnp.float32
        )
        for k, part in enumerate(parts):
            high, mid, low = (
                whole[(3 * k + i) * count : (3 * k + i + 1) * count] for i in range(3)
            )
            part.append(high + (mid + low))
    return [jnp.concatenate(part, axis=1) for part in parts]


def first_product(low, kern, image, base=None):
    width = 512
    for start in range(0, image.shape[1], width):
        here = slice(start, start + width)
        part = jnp.dot(low, kern[:, here], preferred_element_type=jnp.float32)
        image[:, here] = part if base is None else base[:, here] + part


def form_own_kernel(left, right, own, kern, image):
    form(left, right, kern, symmetric=True)
    first_product(own[...].astype(jnp.bfloat16), kern, image)


def form_oth_kernel(left, right, image_own, kern, oth, image):
    form(left, right, kern)
    probes, (rows, deep) = oth.shape[0], right.shape
    low = jnp.concatenate(
        [left[rows + k * probes : rows + (k + 1) * probes, :] for k in range(rows // deep)], axis=1
    )
    oth[...] = low.astype(jnp.float32)
    first_product(low, kern, image, image_own)


def row_sum(first, second):
    return jnp.sum(first * second, axis=1, keepdims=True)


def ahead_kernel(*refs, step):
    if step > 1:
        before_own, table, *refs = refs
    own, image_own, kern_own, ahead, along = refs
    q_own = own[...]
    u_own = image_own[...] + NOISE_LEVEL * q_own
    if step > 1:
        u_own = u_own - table[:, ITERS + step - 2 : ITERS + step - 1] * before_own[...]
    ahead[...], along[...] = product([u_own, q_own], kern_own)


def step_kernel(*refs, step):
    if step > 1:
        before_own, before_oth, table, *refs = refs
    own, oth, image_own, image_oth, ahead, along, kern_oth, *outs = refs
    next_own, next_oth, image, table_out = outs
    lane = lax.broadcasted_iota(jnp.int32, table_out.shape, 1)
    q_own, q_oth = own[...], oth[...]
    w_own = image_own[...] + NOISE_LEVEL * q_own
    w_oth = image_oth[...] + NOISE_LEVEL * q_oth
    u_own, u_oth, last = w_own, w_oth, jnp.zeros(table_out.shape, jnp.float32)
    if step > 1:
        last = table[...]
        beta = last[:, ITERS + step - 2 : ITERS + step - 1]
        u_own = u_own - beta * before_own[...]
        u_oth = u_oth - beta * before_oth[...]
    ahead_oth, along_oth = product([u_oth, q_oth], kern_oth)
    alpha = row_sum(q_own, w_own) + row_sum(q_oth, w_oth)
    r_own, r_oth = u_own - alpha * q_own, u_oth - alpha * q_oth
    beta = jnp.sqrt(
        jnp.maximum(row_sum(r_own, r_own) + row_sum(r_oth, r_oth), 0.0) + FLOOR_BETA
    )
    next_own[...], next_oth[...] = r_own / beta, r_oth / beta
    table_out[...] = jnp.where(
        lane == step - 1, alpha, jnp.where(lane == ITERS + step - 1, beta, last)
    )
    image[...] = (ahead[...] + ahead_oth - alpha * (along[...] + along_oth)) / beta


def finish_kernel(*refs):
    table, oth, image_own, image_oth, *basis = refs[: 4 + ITERS]
    solves, logdet_ref, scale_ref, square = refs[4 + ITERS :]
    probes, local = solves.shape
    root = math.sqrt(2 * oth.shape[1])
    own = basis[-1]
    alpha = row_sum(own[...], image_own[...] + NOISE_LEVEL * own[...]) + row_sum(
        oth[...], image_oth[...] + NOISE_LEVEL * oth[...]
    )
    lane = lax.broadcasted_iota(jnp.int32, table.shape, 1)
    square[...] = jnp.zeros_like(square)
    square[:probes, :] = jnp.where(lane == ITERS - 1, alpha, table[...])
    turned = jnp.transpose(square[...])
    spread = lambda j: jnp.broadcast_to(turned[j : j + 1, :], (8, LANES))
    logdet, coef = quadrature_lanes(
        [spread(j) for j in range(ITERS)], [spread(ITERS + j) for j in range(ITERS - 1)], ITERS
    )
    logdet_ref[...] = logdet[0, :probes]
    scale_ref[...] = 1.0 - NOISE_LEVEL * coef[0, :probes]
    square[:ITERS, :] = coef
    weights = jnp.transpose(square[...])[:probes, :]
    mine = pl.multiple_of(slot_of(0) * local, local)
    total = jnp.zeros((probes, local), jnp.float32)
    for j in range(ITERS):
        total = total + weights[:, j : j + 1] * basis[j][:, pl.ds(mine, local)]
    solves[...] = root * total


def call(kernel, outs, scratch=()):
    return pl.pallas_call(
        kernel,
        out_shape=[jax.ShapeDtypeStruct(shape, dtype) for shape, dtype in outs],
        scratch_shapes=[pltpu.VMEM(shape, dtype) for shape, dtype in scratch],
        compiler_params=pltpu.CompilerParams(vmem_limit_bytes=16 * 2**20),
    )


def replicated(embeds, w_hidden, b_hidden, w_out, probes):
    count, local = probes.shape
    low, wide = jnp.bfloat16, jnp.float32
    block_own = gather_half(head(embeds, w_hidden, b_hidden, w_out, probes))
    half = block_own.shape[0] * local
    deep = w_out.shape[1] + LANES
    vector, square, table = ((count, half), wide), ((half, half), low), ((count, LANES), wide)
    carrier = ((half + count * half // deep, deep), low)
    left, right, own = call(place_kernel, [carrier, ((half, deep), low), vector])(block_own)
    left_oth = partner(left)
    kern_own, image = call(form_own_kernel, [square, vector])(left, right, own)
    kern_oth, oth, image = call(form_oth_kernel, [square, vector, vector])(left_oth, right, image)
    basis, before = [own], ()
    for step in range(1, ITERS):
        image_oth = partner(image)
        ahead, along = call(functools.partial(ahead_kernel, step=step), [vector, vector])(
            *before[::2], own, image, kern_own
        )
        after_own, after_oth, image, rates = call(
            functools.partial(step_kernel, step=step), [vector, vector, vector, table]
        )(*before, own, oth, image, image_oth, ahead, along, kern_oth)
        before = (own, oth, rates)
        own, oth = after_own, after_oth
        basis.append(own)
    return call(
        finish_kernel,
        [((count, local), wide), ((count,), wide), ((count,), wide)],
        [((LANES, LANES), wide)],
    )(rates, oth, image, partner(image), *basis)


def rotate(matrix, vectors, first_idx, second_idx):
    diag_first = matrix[first_idx, first_idx]
    diag_second = matrix[second_idx, second_idx]
    off_value = matrix[first_idx, second_idx]
    half_angle = 0.5 * jnp.arctan2(2.0 * off_value, diag_first - diag_second)
    cosine = jnp.cos(half_angle)
    sine_val = jnp.sin(half_angle)
    row_first = matrix[first_idx]
    row_second = matrix[second_idx]
    matrix = matrix.at[first_idx].set(cosine * row_first + sine_val * row_second)
    matrix = matrix.at[second_idx].set(cosine * row_second - sine_val * row_first)
    col_first = matrix[:, first_idx]
    col_second = matrix[:, second_idx]
    matrix = matrix.at[:, first_idx].set(cosine * col_first + sine_val * col_second)
    matrix = matrix.at[:, second_idx].set(cosine * col_second - sine_val * col_first)
    vec_first = vectors[:, first_idx]
    vec_second = vectors[:, second_idx]
    vectors = vectors.at[:, first_idx].set(cosine * vec_first + sine_val * vec_second)
    vectors = vectors.at[:, second_idx].set(cosine * vec_second - sine_val * vec_first)
    return (matrix, vectors)


def quadrature(alphas, betas):
    tri_order = alphas.shape[0]
    identity = jnp.eye(tri_order, dtype=jnp.float32)
    upper_band = jnp.concatenate([jnp.zeros_like(alphas[:1]), betas], axis=0)
    shifted = jnp.eye(tri_order, k=1, dtype=jnp.float32)[:, :, None] * upper_band[None, :, :]
    matrix = identity[:, :, None] * alphas[None, :, :] + shifted + jnp.transpose(shifted, (1, 0, 2))
    vectors = jnp.broadcast_to(identity[:, :, None], matrix.shape)
    for sweep_index in range(SWEEPS):
        for first_idx in range(tri_order):
            for second_idx in range(first_idx + 1, tri_order):
                matrix, vectors = rotate(matrix, vectors, first_idx, second_idx)
    eigenvalues = jnp.maximum(jnp.sum(matrix * identity[:, :, None], axis=1), EIGEN_FLOOR)
    leading = vectors[0]
    logdet = jnp.sum(jnp.square(leading) * jnp.log(eigenvalues), axis=0)
    coefficients = jnp.sum(vectors * (leading / eigenvalues)[None, :, :], axis=1)
    scale_grad = 1.0 - NOISE_LEVEL * coefficients[0]
    return (logdet, scale_grad, coefficients)


def kernel_block(row_feats, row_norms, col_block, norm_block):
    inner = lax.dot_general(
        row_feats, col_block, (((1,), (1,)), ((), ())), preferred_element_type=jnp.float32
    )
    distance = row_norms[:, None] + norm_block[None, :] - 2.0 * inner
    return jnp.exp(-jnp.maximum(distance, 0.0) * INV_WIDTH).astype(jnp.bfloat16)


def block_width():
    return 512


def form_tile(row_feats, row_norms, col_feats, col_norms):
    total_cols = col_feats.shape[0]
    step_cols = block_width()
    block_count = total_cols // step_cols

    def one_block(block_index, tile):
        offset = block_index * step_cols
        col_block = lax.dynamic_slice_in_dim(col_feats, offset, step_cols, 0)
        norm_block = lax.dynamic_slice_in_dim(col_norms, offset, step_cols, 0)
        block = kernel_block(row_feats, row_norms, col_block, norm_block)
        return lax.dynamic_update_slice_in_dim(tile, block, offset, 1)

    empty = jnp.zeros((row_feats.shape[0], total_cols), jnp.bfloat16)
    return lax.fori_loop(0, block_count, one_block, empty)


def apply_kernel(vectors_low, tile):
    partial_value = lax.dot_general(
        lax.all_gather(vectors_low, "row", axis=1, tiled=True),
        tile,
        (((1,), (1,)), ((), ())),
        preferred_element_type=jnp.float32,
    )
    return lax.psum_scatter(partial_value, "grp", scatter_dimension=1, tiled=True)


def distributed(embeds, w_hidden, b_hidden, w_out, probes):
    hidden = jax.nn.gelu(
        jnp.dot(embeds, w_hidden, preferred_element_type=jnp.float32) + b_hidden
    ).astype(jnp.bfloat16)
    features = jnp.dot(hidden, w_out, preferred_element_type=jnp.float32).astype(jnp.bfloat16)
    row_feats = lax.all_gather(features, "grp", axis=0, tiled=True)
    col_feats = lax.all_gather(features, "row", axis=0, tiled=True)
    row_norms = jnp.sum(jnp.square(row_feats.astype(jnp.float32)), axis=1)
    col_norms = jnp.sum(jnp.square(col_feats.astype(jnp.float32)), axis=1)
    tile = form_tile(row_feats, row_norms, col_feats, col_norms)
    total_rows = probes.shape[1] * lax.axis_size("grp") * lax.axis_size("row")
    scale_root = math.sqrt(total_rows)
    current = (2 * probes - 1).astype(jnp.float32) / scale_root
    previous = jnp.zeros_like(current)
    beta_prev = jnp.zeros((current.shape[0],), jnp.float32)
    basis_list = []
    alpha_list = []
    beta_list = []
    for iteration in range(ITERS):
        kernel_image = apply_kernel(current.astype(jnp.bfloat16), tile) + NOISE_LEVEL * current
        moments = jnp.stack(
            [
                jnp.sum(current * kernel_image, axis=1),
                jnp.sum(kernel_image * kernel_image, axis=1),
                jnp.sum(previous * kernel_image, axis=1),
                jnp.sum(current * previous, axis=1),
                jnp.sum(current * current, axis=1),
                jnp.sum(previous * previous, axis=1),
            ]
        )
        moments = lax.psum(moments, ("grp", "row"))
        alpha_now = moments[0]
        residual_sq = (
            moments[1]
            + alpha_now * alpha_now * moments[4]
            + beta_prev * beta_prev * moments[5]
            - 2.0 * alpha_now * moments[0]
            - 2.0 * beta_prev * moments[2]
            + 2.0 * alpha_now * beta_prev * moments[3]
        )
        residual = kernel_image - alpha_now[:, None] * current - beta_prev[:, None] * previous
        basis_list.append(current)
        alpha_list.append(alpha_now)
        if iteration + 1 < ITERS:
            beta_now = jnp.sqrt(jnp.maximum(residual_sq, 0.0) + FLOOR_BETA)
            beta_list.append(beta_now)
            previous = current
            current = residual / beta_now[:, None]
            beta_prev = beta_now
    logdet, scale_grad, coefficients = quadrature(jnp.stack(alpha_list), jnp.stack(beta_list))
    solves = scale_root * jnp.einsum("jp,jpn->pn", coefficients, jnp.stack(basis_list))
    return (solves, logdet, scale_grad)


def power_of_two(value):
    return value & (value - 1) == 0


def solution(mesh):
    groups, lines = mesh.shape["grp"], mesh.shape["row"]

    def local(embeds, w_hidden, b_hidden, w_out, probes):
        rows = embeds.shape[0] * groups * lines
        fits = (
            rows * rows <= KERNEL_BYTES
            and lines % 2 == 0
            and power_of_two(groups)
            and power_of_two(lines)
            and probes.shape[1] == LANES
            and w_out.shape[1] == LANES
            and probes.shape[0] % 16 == 0
        )
        step = replicated if fits else distributed
        return step(embeds, w_hidden, b_hidden, w_out, probes)

    return jax.shard_map(
        local,
        mesh=mesh,
        in_specs=(P(("grp", "row"), None), P(), P(), P(), P(None, ("grp", "row"))),
        out_specs=(P(None, ("grp", "row")), P(), P()),
        check_vma=False,
    )
```

```python
import functools
import math

import jax
import jax.numpy as jnp
from jax import lax
from jax.experimental import pallas as pl
from jax.experimental.pallas import tpu as pltpu
from jax.sharding import PartitionSpec as P

ITERS = 8
SWEEPS = 6
INV_WIDTH = 1.0 / 12.0
NOISE_LEVEL = 0.5
FLOOR_BETA = 0.01
EIGEN_FLOOR = 0.25
LANES = 128
TINY = 1e-15
KERNEL_BYTES = 40 * 2**20


def head_kernel(*refs):
    sources, (out_ref, *places, sems) = refs[:5], refs[5:]
    copies = [
        pltpu.make_async_copy(source, place, sems.at[k])
        for k, (source, place) in enumerate(zip(sources, places))
    ]
    for copy in copies:
        copy.start()
    embeds, w_hidden, b_hidden, w_out, probes = places
    rows = embeds.shape[0]
    for copy in copies:
        copy.wait()
    hidden = jax.nn.gelu(
        jnp.dot(embeds[...], w_hidden[...], preferred_element_type=jnp.float32)
        + b_hidden[...][None, :]
    ).astype(jnp.bfloat16)
    out_ref[:rows, :] = jnp.dot(
        hidden, w_out[...], preferred_element_type=jnp.float32
    ).astype(jnp.bfloat16)
    out_ref[rows:, :] = probes[...].astype(jnp.float32).astype(jnp.bfloat16)


def head(*arrays):
    embeds, w_out, probes = arrays[0], arrays[3], arrays[4]
    shape = (embeds.shape[0] + probes.shape[0], w_out.shape[1])
    return pl.pallas_call(
        head_kernel,
        out_shape=pltpu.VMEM(shape, jnp.bfloat16),
        in_specs=[pl.BlockSpec(memory_space=pl.ANY)] * len(arrays),
        out_specs=pl.BlockSpec(memory_space=pltpu.VMEM),
        scratch_shapes=[pltpu.VMEM(a.shape, a.dtype) for a in arrays]
        + [pltpu.SemaphoreType.DMA((len(arrays),))],
    )(*arrays)


def swap(value, axis, flip):
    size = lax.axis_size(axis)
    return lax.ppermute(value, axis, [(i, i ^ flip) for i in range(size)])


def gather_half(block):
    def spread(value, axis, stride):
        far = range(1, lax.axis_size(axis) // stride)
        return jnp.concatenate([value] + [swap(value, axis, stride * k) for k in far])

    return spread(spread(block[None], "row", 2), "grp", 1)


def partner(value):
    return swap(value, "row", 1)


def pairs_of_round(order, turn):
    ring = order - 1
    pairs = [(ring, turn)]
    for gap in range(1, order // 2):
        pairs.append(((turn + gap) % ring, (turn - gap) % ring))
    return [tuple(sorted(pair)) for pair in pairs]


def jacobi_round(entries, columns, pairs):
    entries, columns = dict(entries), list(columns)

    def key(i, j):
        return (i, j) if i <= j else (j, i)

    turns = []
    for p, q in pairs:
        off = entries[p, q]
        gap = entries[q, q] - entries[p, p]
        size = jnp.abs(gap) + TINY
        square = size * size + 4.0 * (off * off)
        inverse = lax.rsqrt(square)
        cos_square = 0.5 + 0.5 * size * inverse
        secant = lax.rsqrt(cos_square)
        signed = jnp.where(gap >= 0.0, inverse, -inverse)
        turns.append((cos_square * secant, off * signed * secant, square * signed))
    for (p, q), (cosine, sine, width) in zip(pairs, turns):
        middle = entries[p, p] + entries[q, q]
        entries[p, p] = 0.5 * (middle - width)
        entries[q, q] = 0.5 * (middle + width)
        entries[p, q] = jnp.zeros_like(width)
        col_p, col_q = columns[p], columns[q]
        columns[p] = cosine * col_p - sine * col_q
        columns[q] = sine * col_p + cosine * col_q
    for a in range(len(pairs)):
        for b in range(a + 1, len(pairs)):
            (p, q), (r, s) = pairs[a], pairs[b]
            cos_a, sin_a, _ = turns[a]
            cos_b, sin_b, _ = turns[b]
            pr, ps = entries[key(p, r)], entries[key(p, s)]
            qr, qs = entries[key(q, r)], entries[key(q, s)]
            pr, qr = cos_a * pr - sin_a * qr, sin_a * pr + cos_a * qr
            ps, qs = cos_a * ps - sin_a * qs, sin_a * ps + cos_a * qs
            pr, ps = cos_b * pr - sin_b * ps, sin_b * pr + cos_b * ps
            qr, qs = cos_b * qr - sin_b * qs, sin_b * qr + cos_b * qs
            entries[key(p, r)], entries[key(p, s)] = pr, ps
            entries[key(q, r)], entries[key(q, s)] = qr, qs
    return entries, columns


def quadrature_lanes(alphas, betas, order):
    shape = alphas[0].shape
    keys = [(i, j) for i in range(order) for j in range(i, order)]
    entries = {}
    for i, j in keys:
        if i == j:
            entries[i, j] = alphas[i]
        elif j == i + 1:
            entries[i, j] = betas[i]
        else:
            entries[i, j] = jnp.zeros(shape, jnp.float32)
    sublane = lax.broadcasted_iota(jnp.int32, shape, 0)
    columns = [jnp.where(sublane == k, 1.0, 0.0).astype(jnp.float32) for k in range(order)]

    def sweep(_, state):
        values, columns = state
        entries = dict(zip(keys, values))
        for turn in range(order - 1):
            entries, columns = jacobi_round(entries, columns, pairs_of_round(order, turn))
        return tuple(entries[k] for k in keys), tuple(columns)

    values, columns = lax.fori_loop(
        0, SWEEPS, sweep, (tuple(entries[k] for k in keys), tuple(columns))
    )
    entries = dict(zip(keys, values))
    logdet = jnp.zeros((1, shape[1]), jnp.float32)
    coef = jnp.zeros(shape, jnp.float32)
    for k in range(order):
        eigen = jnp.maximum(entries[k, k][:1], EIGEN_FLOOR)
        leading = columns[k][:1]
        logdet = logdet + leading * leading * jnp.log(eigen)
        coef = coef + columns[k] * (leading / eigen)
    return logdet, coef


def split3(value):
    high = value.astype(jnp.bfloat16)
    rest = value - high.astype(jnp.float32)
    mid = rest.astype(jnp.bfloat16)
    low = (rest - mid.astype(jnp.float32)).astype(jnp.bfloat16)
    return high, mid, low


def slot_of(index):
    lines = lax.axis_size("row") // 2
    line, group = lax.axis_index("row") // 2, lax.axis_index("grp")
    return (group ^ (index // lines)) * lines + (line ^ (index % lines))


def place_kernel(blocks, left, right, start_vec):
    count, block_rows, feat = blocks.shape
    probes = start_vec.shape[0]
    local = block_rows - probes
    rows, deep = right.shape
    root = math.sqrt(2 * rows)
    lane = lax.broadcasted_iota(jnp.int32, (local, LANES), 1)
    adder = jnp.full((2 * feat, LANES), -0.5, jnp.bfloat16)
    ones = jnp.where((lane < 3) | ((lane >= 6) & (lane < 9)), 1.0, 0.0)

    def rounded(value):
        return value.astype(jnp.bfloat16).astype(jnp.float32)

    def place(index, carry):
        start = pl.multiple_of(slot_of(index) * local, local)
        here = pl.ds(start, local)
        feats = blocks[index, :local, :]
        wide = feats.astype(jnp.float32)
        square = wide * wide
        high = square.astype(jnp.bfloat16)
        low = (square - high.astype(jnp.float32)).astype(jnp.bfloat16)
        total = jnp.dot(
            jnp.concatenate([high, low], axis=1), adder, preferred_element_type=jnp.float32
        )
        rest = total - rounded(total)
        pieces = jnp.where(lane == 3, total, jnp.where(lane == 4, rest, rest - rounded(rest)))
        pieces = jnp.where((lane >= 3) & (lane < 6), pieces, ones)
        left[here, :feat] = feats
        left[here, feat:] = pieces.astype(jnp.bfloat16)
        right[here, :feat] = feats
        right[here, feat:] = pltpu.roll(pieces, LANES - 3, 1).astype(jnp.bfloat16)
        bits = blocks[index, local:, :].astype(jnp.float32)
        start_vec[:, here] = (2.0 * bits - 1.0) / root
        return carry

    lax.fori_loop(0, count, place, 0, unroll=16)
    for k in range(rows // deep):
        left[rows + k * probes : rows + (k + 1) * probes, :] = start_vec[
            :, k * deep : (k + 1) * deep
        ].astype(jnp.bfloat16)


def form(left, right, kern, symmetric=False):
    size = 256 if symmetric else 1024
    rows = right.shape[0]
    for start in range(0, rows, size):
        block = right[start : start + size, :]
        for top in range(start if symmetric else 0, rows, size):
            inner = lax.dot_general(
                left[top : top + size, :],
                block,
                (((1,), (1,)), ((), ())),
                preferred_element_type=jnp.float32,
            )
            tile = jnp.exp2(
                jnp.minimum(inner, 0.0) * (2.0 * INV_WIDTH * math.log2(math.e))
            ).astype(jnp.bfloat16)
            kern[top : top + size, start : start + size] = tile
            if symmetric and top > start:
                kern[start : start + size, top : top + size] = tile.T


def product(vectors, kern):
    count = vectors[0].shape[0]
    pieces = jnp.concatenate([piece for vector in vectors for piece in split3(vector)])
    width = 1024
    parts = [[] for _ in vectors]
    for start in range(0, kern.shape[1], width):
        whole = jnp.dot(
            pieces, kern[:, start : start + width], preferred_element_type=jnp.float32
        )
        for k, part in enumerate(parts):
            high, mid, low = (
                whole[(3 * k + i) * count : (3 * k + i + 1) * count] for i in range(3)
            )
            part.append(high + (mid + low))
    return [jnp.concatenate(part, axis=1) for part in parts]


def first_product(low, kern, image, base=None):
    width = 512
    for start in range(0, image.shape[1], width):
        here = slice(start, start + width)
        part = jnp.dot(low, kern[:, here], preferred_element_type=jnp.float32)
        image[:, here] = part if base is None else base[:, here] + part


def form_own_kernel(left, right, own, kern, image):
    form(left, right, kern, symmetric=True)
    first_product(own[...].astype(jnp.bfloat16), kern, image)


def form_oth_kernel(left, right, image_own, kern, oth, image):
    form(left, right, kern)
    probes, (rows, deep) = oth.shape[0], right.shape
    low = jnp.concatenate(
        [left[rows + k * probes : rows + (k + 1) * probes, :] for k in range(rows // deep)], axis=1
    )
    oth[...] = low.astype(jnp.float32)
    first_product(low, kern, image, image_own)


def row_sum(first, second):
    return jnp.sum(first * second, axis=1, keepdims=True)


def ahead_kernel(*refs, step):
    if step > 1:
        before_own, table, *refs = refs
    own, image_own, kern_own, ahead, along = refs
    q_own = own[...]
    u_own = image_own[...] + NOISE_LEVEL * q_own
    if step > 1:
        u_own = u_own - table[:, ITERS + step - 2 : ITERS + step - 1] * before_own[...]
    ahead[...], along[...] = product([u_own, q_own], kern_own)


def step_kernel(*refs, step):
    if step > 1:
        before_own, before_oth, table, *refs = refs
    own, oth, image_own, image_oth, ahead, along, kern_oth, *outs = refs
    next_own, next_oth, image, table_out = outs
    lane = lax.broadcasted_iota(jnp.int32, table_out.shape, 1)
    q_own, q_oth = own[...], oth[...]
    w_own = image_own[...] + NOISE_LEVEL * q_own
    w_oth = image_oth[...] + NOISE_LEVEL * q_oth
    u_own, u_oth, last = w_own, w_oth, jnp.zeros(table_out.shape, jnp.float32)
    if step > 1:
        last = table[...]
        beta = last[:, ITERS + step - 2 : ITERS + step - 1]
        u_own = u_own - beta * before_own[...]
        u_oth = u_oth - beta * before_oth[...]
    ahead_oth, along_oth = product([u_oth, q_oth], kern_oth)
    alpha = row_sum(q_own, w_own) + row_sum(q_oth, w_oth)
    r_own, r_oth = u_own - alpha * q_own, u_oth - alpha * q_oth
    beta = jnp.sqrt(
        jnp.maximum(row_sum(r_own, r_own) + row_sum(r_oth, r_oth), 0.0) + FLOOR_BETA
    )
    next_own[...], next_oth[...] = r_own / beta, r_oth / beta
    table_out[...] = jnp.where(
        lane == step - 1, alpha, jnp.where(lane == ITERS + step - 1, beta, last)
    )
    image[...] = (ahead[...] + ahead_oth - alpha * (along[...] + along_oth)) / beta


def finish_kernel(*refs):
    table, oth, image_own, image_oth, *basis = refs[: 4 + ITERS]
    solves, logdet_ref, scale_ref, square = refs[4 + ITERS :]
    probes, local = solves.shape
    root = math.sqrt(2 * oth.shape[1])
    own = basis[-1]
    alpha = row_sum(own[...], image_own[...] + NOISE_LEVEL * own[...]) + row_sum(
        oth[...], image_oth[...] + NOISE_LEVEL * oth[...]
    )
    lane = lax.broadcasted_iota(jnp.int32, table.shape, 1)
    square[...] = jnp.zeros_like(square)
    square[:probes, :] = jnp.where(lane == ITERS - 1, alpha, table[...])
    turned = jnp.transpose(square[...])
    spread = lambda j: jnp.broadcast_to(turned[j : j + 1, :], (8, LANES))
    logdet, coef = quadrature_lanes(
        [spread(j) for j in range(ITERS)], [spread(ITERS + j) for j in range(ITERS - 1)], ITERS
    )
    logdet_ref[...] = logdet[0, :probes]
    scale_ref[...] = 1.0 - NOISE_LEVEL * coef[0, :probes]
    square[:ITERS, :] = coef
    weights = jnp.transpose(square[...])[:probes, :]
    mine = pl.multiple_of(slot_of(0) * local, local)
    total = jnp.zeros((probes, local), jnp.float32)
    for j in range(ITERS):
        total = total + weights[:, j : j + 1] * basis[j][:, pl.ds(mine, local)]
    solves[...] = root * total


def call(kernel, outs, scratch=()):
    return pl.pallas_call(
        kernel,
        out_shape=[jax.ShapeDtypeStruct(shape, dtype) for shape, dtype in outs],
        scratch_shapes=[pltpu.VMEM(shape, dtype) for shape, dtype in scratch],
        compiler_params=pltpu.CompilerParams(vmem_limit_bytes=16 * 2**20),
    )


def replicated(embeds, w_hidden, b_hidden, w_out, probes):
    count, local = probes.shape
    low, wide = jnp.bfloat16, jnp.float32
    block_own = gather_half(head(embeds, w_hidden, b_hidden, w_out, probes))
    half = block_own.shape[0] * local
    deep = w_out.shape[1] + LANES
    vector, square, table = ((count, half), wide), ((half, half), low), ((count, LANES), wide)
    carrier = ((half + count * half // deep, deep), low)
    left, right, own = call(place_kernel, [carrier, ((half, deep), low), vector])(block_own)
    left_oth = partner(left)
    kern_own, image = call(form_own_kernel, [square, vector])(left, right, own)
    kern_oth, oth, image = call(form_oth_kernel, [square, vector, vector])(left_oth, right, image)
    basis, before = [own], ()
    for step in range(1, ITERS):
        image_oth = partner(image)
        ahead, along = call(functools.partial(ahead_kernel, step=step), [vector, vector])(
            *before[::2], own, image, kern_own
        )
        after_own, after_oth, image, rates = call(
            functools.partial(step_kernel, step=step), [vector, vector, vector, table]
        )(*before, own, oth, image, image_oth, ahead, along, kern_oth)
        before = (own, oth, rates)
        own, oth = after_own, after_oth
        basis.append(own)
    return call(
        finish_kernel,
        [((count, local), wide), ((count,), wide), ((count,), wide)],
        [((LANES, LANES), wide)],
    )(rates, oth, image, partner(image), *basis)


def rotate(matrix, vectors, first_idx, second_idx):
    diag_first = matrix[first_idx, first_idx]
    diag_second = matrix[second_idx, second_idx]
    off_value = matrix[first_idx, second_idx]
    half_angle = 0.5 * jnp.arctan2(2.0 * off_value, diag_first - diag_second)
    cosine = jnp.cos(half_angle)
    sine_val = jnp.sin(half_angle)
    row_first = matrix[first_idx]
    row_second = matrix[second_idx]
    matrix = matrix.at[first_idx].set(cosine * row_first + sine_val * row_second)
    matrix = matrix.at[second_idx].set(cosine * row_second - sine_val * row_first)
    col_first = matrix[:, first_idx]
    col_second = matrix[:, second_idx]
    matrix = matrix.at[:, first_idx].set(cosine * col_first + sine_val * col_second)
    matrix = matrix.at[:, second_idx].set(cosine * col_second - sine_val * col_first)
    vec_first = vectors[:, first_idx]
    vec_second = vectors[:, second_idx]
    vectors = vectors.at[:, first_idx].set(cosine * vec_first + sine_val * vec_second)
    vectors = vectors.at[:, second_idx].set(cosine * vec_second - sine_val * vec_first)
    return (matrix, vectors)


def quadrature(alphas, betas):
    tri_order = alphas.shape[0]
    identity = jnp.eye(tri_order, dtype=jnp.float32)
    upper_band = jnp.concatenate([jnp.zeros_like(alphas[:1]), betas], axis=0)
    shifted = jnp.eye(tri_order, k=1, dtype=jnp.float32)[:, :, None] * upper_band[None, :, :]
    matrix = identity[:, :, None] * alphas[None, :, :] + shifted + jnp.transpose(shifted, (1, 0, 2))
    vectors = jnp.broadcast_to(identity[:, :, None], matrix.shape)
    for sweep_index in range(SWEEPS):
        for first_idx in range(tri_order):
            for second_idx in range(first_idx + 1, tri_order):
                matrix, vectors = rotate(matrix, vectors, first_idx, second_idx)
    eigenvalues = jnp.maximum(jnp.sum(matrix * identity[:, :, None], axis=1), EIGEN_FLOOR)
    leading = vectors[0]
    logdet = jnp.sum(jnp.square(leading) * jnp.log(eigenvalues), axis=0)
    coefficients = jnp.sum(vectors * (leading / eigenvalues)[None, :, :], axis=1)
    scale_grad = 1.0 - NOISE_LEVEL * coefficients[0]
    return (logdet, scale_grad, coefficients)


def kernel_block(row_feats, row_norms, col_block, norm_block):
    inner = lax.dot_general(
        row_feats, col_block, (((1,), (1,)), ((), ())), preferred_element_type=jnp.float32
    )
    distance = row_norms[:, None] + norm_block[None, :] - 2.0 * inner
    return jnp.exp(-jnp.maximum(distance, 0.0) * INV_WIDTH).astype(jnp.bfloat16)


def block_width():
    return 512


def form_tile(row_feats, row_norms, col_feats, col_norms):
    total_cols = col_feats.shape[0]
    step_cols = block_width()
    block_count = total_cols // step_cols

    def one_block(block_index, tile):
        offset = block_index * step_cols
        col_block = lax.dynamic_slice_in_dim(col_feats, offset, step_cols, 0)
        norm_block = lax.dynamic_slice_in_dim(col_norms, offset, step_cols, 0)
        block = kernel_block(row_feats, row_norms, col_block, norm_block)
        return lax.dynamic_update_slice_in_dim(tile, block, offset, 1)

    empty = jnp.zeros((row_feats.shape[0], total_cols), jnp.bfloat16)
    return lax.fori_loop(0, block_count, one_block, empty)


def apply_kernel(vectors_low, tile):
    partial_value = lax.dot_general(
        lax.all_gather(vectors_low, "row", axis=1, tiled=True),
        tile,
        (((1,), (1,)), ((), ())),
        preferred_element_type=jnp.float32,
    )
    return lax.psum_scatter(partial_value, "grp", scatter_dimension=1, tiled=True)


def distributed(embeds, w_hidden, b_hidden, w_out, probes):
    hidden = jax.nn.gelu(
        jnp.dot(embeds, w_hidden, preferred_element_type=jnp.float32) + b_hidden
    ).astype(jnp.bfloat16)
    features = jnp.dot(hidden, w_out, preferred_element_type=jnp.float32).astype(jnp.bfloat16)
    row_feats = lax.all_gather(features, "grp", axis=0, tiled=True)
    col_feats = lax.all_gather(features, "row", axis=0, tiled=True)
    row_norms = jnp.sum(jnp.square(row_feats.astype(jnp.float32)), axis=1)
    col_norms = jnp.sum(jnp.square(col_feats.astype(jnp.float32)), axis=1)
    tile = form_tile(row_feats, row_norms, col_feats, col_norms)
    total_rows = probes.shape[1] * lax.axis_size("grp") * lax.axis_size("row")
    scale_root = math.sqrt(total_rows)
    current = (2 * probes - 1).astype(jnp.float32) / scale_root
    previous = jnp.zeros_like(current)
    beta_prev = jnp.zeros((current.shape[0],), jnp.float32)
    basis_list = []
    alpha_list = []
    beta_list = []
    for iteration in range(ITERS):
        kernel_image = apply_kernel(current.astype(jnp.bfloat16), tile) + NOISE_LEVEL * current
        moments = jnp.stack(
            [
                jnp.sum(current * kernel_image, axis=1),
                jnp.sum(kernel_image * kernel_image, axis=1),
                jnp.sum(previous * kernel_image, axis=1),
                jnp.sum(current * previous, axis=1),
                jnp.sum(current * current, axis=1),
                jnp.sum(previous * previous, axis=1),
            ]
        )
        moments = lax.psum(moments, ("grp", "row"))
        alpha_now = moments[0]
        residual_sq = (
            moments[1]
            + alpha_now * alpha_now * moments[4]
            + beta_prev * beta_prev * moments[5]
            - 2.0 * alpha_now * moments[0]
            - 2.0 * beta_prev * moments[2]
            + 2.0 * alpha_now * beta_prev * moments[3]
        )
        residual = kernel_image - alpha_now[:, None] * current - beta_prev[:, None] * previous
        basis_list.append(current)
        alpha_list.append(alpha_now)
        if iteration + 1 < ITERS:
            beta_now = jnp.sqrt(jnp.maximum(residual_sq, 0.0) + FLOOR_BETA)
            beta_list.append(beta_now)
            previous = current
            current = residual / beta_now[:, None]
            beta_prev = beta_now
    logdet, scale_grad, coefficients = quadrature(jnp.stack(alpha_list), jnp.stack(beta_list))
    solves = scale_root * jnp.einsum("jp,jpn->pn", coefficients, jnp.stack(basis_list))
    return (solves, logdet, scale_grad)


def power_of_two(value):
    return value & (value - 1) == 0


def solution(mesh):
    groups, lines = mesh.shape["grp"], mesh.shape["row"]

    def local(embeds, w_hidden, b_hidden, w_out, probes):
        rows = embeds.shape[0] * groups * lines
        fits = (
            rows * rows <= KERNEL_BYTES
            and lines % 2 == 0
            and power_of_two(groups)
            and power_of_two(lines)
            and probes.shape[1] == LANES
            and w_out.shape[1] == LANES
            and probes.shape[0] % 16 == 0
        )
        step = replicated if fits else distributed
        return step(embeds, w_hidden, b_hidden, w_out, probes)

    return jax.shard_map(
        local,
        mesh=mesh,
        in_specs=(P(("grp", "row"), None), P(), P(), P(), P(None, ("grp", "row"))),
        out_specs=(P(None, ("grp", "row")), P(), P()),
        check_vma=False,
    )
```
